256 devices in a mesh: panel: 64 (over z, x, core), obs: 4 (over y).
Axes of the slice: x: 4, y: 4, z: 8, core: 2. Of those that a mesh axis runs over, the one named last changes fastest.
Arguments:
- samples: bfloat16 [1024, 4, 32768], P(('panel', 'obs')), may hold values from -6 to 6
- panel_position: float32 [3, 32768], P(None, 'panel'), may hold values from -1 to 1
- panel_area: float32 [32768], P('panel'), may hold values from 0.5 to 2
- panel_counts: int32 [256], P('panel'), may hold values from 1 to 128
- obs_position: float32 [3, 1024], P(None, 'obs'), may hold values from -12 to 12, as said below
- freq_bins: int32 [32], replicated, may hold values from 1 to 511
Outputs:
- far_pressure: float32 [2, 32, 1024], P(None, None, ('obs', 'panel'))
The draws below stay inside these ranges and needn't reach their ends.
Inputs may be any that keep to these rules, and one draw needn't show every extreme that they name: `obs_position`: observers lie at distances 6 to 12 from the anchor.
All inputs are finite; a program needn't handle non-finite values.
Results may differ from the reference program's by a relative error of at most 0.0027.
Values may be sent and summed in bfloat16 or wider, within the bound.
No kernel may reach another device: no remote copies, remote signals or barrier semaphores. Data moves between devices by JAX's collectives and lax.ppermute only.
A program may use at most 64 MiB of HBM per device.

```python
import math
import jax
import jax.numpy as jnp
from jax import lax

TIME = 1024
NF = 32
FBLK = 4
PANELS = 32768
OBS = 1024
NBLK = 256


def draw_obs_position(key, part):
    subkeys = jax.random.split(jax.random.fold_in(key, 11), 3)
    height = jax.random.uniform(subkeys[0], (OBS,), jnp.float32, -1.0, 1.0)
    azimuth = jax.random.uniform(subkeys[1], (OBS,), jnp.float32, -math.pi, math.pi)
    radius = jax.random.uniform(subkeys[2], (OBS,), jnp.float32, 6.0, 12.0)
    cycle_radius = radius * jnp.sqrt(jnp.maximum(1.0 - height * height, 0.0))
    return jnp.stack([cycle_radius * jnp.cos(azimuth), cycle_radius * jnp.sin(azimuth), radius * height])


def touch_ends(array, stream_key, smallest, top_value):
    longest = array.shape.index(max(array.shape))
    spots = []
    for shift in (0, 1):
        where = [jax.random.randint(jax.random.fold_in(stream_key, axis), (), 0, length) for axis, length in enumerate(array.shape)]
        where[longest] = (where[longest] + shift) % array.shape[longest]
        spots.append(tuple(where))
    return array.at[spots[0]].set(smallest).at[spots[1]].set(top_value)


def steps_of(own_key, shape, shards, smallest, top_value):
    loudness = 1.0
    for position, shards_of in shards:
        draws = jax.random.uniform(jax.random.fold_in(jax.random.fold_in(own_key, 6), position), (shards_of,), jnp.float32, smallest / len(shards), top_value / len(shards))
        loudness = loudness * jnp.repeat(jnp.exp(draws), shape[position] // shards_of).reshape((-1,) + (1,) * (len(shape) - 1 - position))
    return loudness


def centred(key, shape, deviation, most, cuts=(), kind=jnp.bfloat16):
    level = steps_of(key, shape, cuts, -0.22, 0.18) if cuts else 1.0
    values = jax.random.normal(key, shape, jnp.float32) * deviation * level
    return jnp.minimum(jnp.maximum(values, -most), most).astype(kind)


def setup_inputs(seed: int = 0) -> dict:
    splits = jax.random.split(jax.random.key(seed), 7)
    return {
        "samples": centred(splits[0], (TIME, 4, PANELS), 1.0, 6.0, ((0, 256),)),
        "panel_position": jnp.clip(jax.random.uniform(splits[1], (3, PANELS), jnp.float32, -1.0, 1.0) * steps_of(splits[1], (3, PANELS), ((1, 64),), -0.4, 0.0), -1.0, 1.0),
        "panel_area": jnp.clip(jnp.exp(math.log(2.0) - 1.3862944 * jax.random.uniform(splits[2], (PANELS,), jnp.float32) ** steps_of(splits[2], (PANELS,), ((0, 64),), -0.2, 0.2)), 0.5, 2.0),
        "panel_counts": touch_ends(jax.random.randint(splits[3], (NBLK,), 1, 129), jax.random.fold_in(splits[3], 1), 1, 128).astype(jnp.int32),
        "obs_position": draw_obs_position(jax.random.fold_in(splits[6], 71), 0),
        "freq_bins": touch_ends(jax.random.randint(splits[5], (NF,), 1, TIME // 2), jax.random.fold_in(splits[5], 1), 1, (TIME // 2) - 1).astype(jnp.int32),
    }


SPACING = 0.1

def make_table(time_rows, freq_bins):
    phase_index = freq_bins[None, :] * time_rows[:, None] % TIME
    angle_arg = 2.0 * math.pi / TIME * phase_index.astype(jnp.float32)
    window = 0.5 - 0.5 * jnp.cos(2.0 * math.pi / TIME * time_rows.astype(jnp.float32))
    weight = 2.0 / TIME * window[:, None]
    return jnp.concatenate([weight * jnp.cos(angle_arg), -weight * jnp.sin(angle_arg)], axis=1).astype(jnp.bfloat16)

def live_rows(counts):
    lane_ids = jnp.arange(128, dtype=jnp.int32)
    return (lane_ids[None, :] < counts[:, None]).astype(jnp.float32).reshape(-1)

def radiate(obs_position, panel_position, panel_area, spectra, freq_bins):
    offset = obs_position[:, :, None] - panel_position[:, None, :]
    distance = jnp.sqrt(lax.optimization_barrier(jnp.sum(offset * offset, axis=0)))
    inverse = 1.0 / distance
    unit_dir = offset * inverse[None]
    green_scale = panel_area[None, :] * inverse * (1.0 / (4.0 * math.pi))
    freq_count = freq_bins.shape[0]
    real_blocks = spectra[:freq_count].reshape(freq_count // FBLK, FBLK, 4, -1)
    imag_blocks = spectra[freq_count:].reshape(freq_count // FBLK, FBLK, 4, -1)
    bin_blocks = freq_bins.reshape(freq_count // FBLK, FBLK)

    def one_block(block_items):
        real_src, imag_src, bin_block = block_items
        wavenumber = (2.0 * math.pi / (TIME * SPACING) * bin_block.astype(jnp.float32))[:, None, None]
        radial_real = lax.optimization_barrier(jnp.sum(unit_dir[None] * real_src[:, 1:, None, :], axis=1))
        radial_imag = lax.optimization_barrier(jnp.sum(unit_dir[None] * imag_src[:, 1:, None, :], axis=1))
        source_real = -wavenumber * imag_src[:, 0][:, None, :] + radial_real * inverse[None] - wavenumber * radial_imag
        source_imag = wavenumber * real_src[:, 0][:, None, :] + wavenumber * radial_real + radial_imag * inverse[None]
        phase_arg = wavenumber * distance[None]
        cosine = jnp.cos(phase_arg)
        sine_part = jnp.sin(phase_arg)
        out_real = lax.optimization_barrier(jnp.sum(green_scale[None] * (cosine * source_real + sine_part * source_imag), axis=2))
        out_imag = lax.optimization_barrier(jnp.sum(green_scale[None] * (cosine * source_imag - sine_part * source_real), axis=2))
        return jnp.stack([out_real, out_imag])
    result = lax.map(one_block, (real_blocks, imag_blocks, bin_blocks))
    return jnp.transpose(result, (1, 0, 2, 3)).reshape(2, freq_count, -1)

def reference(samples, panel_position, panel_area, panel_counts, obs_position, freq_bins):
    time_rows = jnp.arange(TIME, dtype=jnp.int32)
    window_table = make_table(time_rows, freq_bins)
    flat_samples = samples.reshape(TIME, -1)
    raw_spectra = lax.dot_general(window_table, flat_samples, (((0,), (0,)), ((), ())), preferred_element_type=jnp.float32)
    sources = raw_spectra.reshape(2 * NF, 4, PANELS) * live_rows(panel_counts)[None, None, :]

    def accumulate(running, block_index):
        first_row = block_index * 1024
        slice_spectra = lax.dynamic_slice_in_dim(sources, first_row, 1024, 2)
        block_position = lax.dynamic_slice_in_dim(panel_position, first_row, 1024, 1)
        block_area = lax.dynamic_slice_in_dim(panel_area, first_row, 1024, 0)
        return (running + radiate(obs_position, block_position, block_area, slice_spectra, freq_bins), None)
    running, _ = lax.scan(accumulate, jnp.zeros((2, NF, OBS), jnp.float32), jnp.arange(PANELS // 1024, dtype=jnp.int32))
    return running
```

```python
import math

import jax
import jax.numpy as jnp
from jax import lax
from jax.experimental import pallas as pl
from jax.experimental.pallas import tpu as pltpu
from jax.sharding import PartitionSpec as P

TIME = 1024
NF = 32
SPACING = 0.1
LANES = 128
CHANNELS = 4
BLOCKS = 8
TILE = 32
DEPTH = 8
SLOT = 16

SIN_COEFFS = (
    4.442882919199695,
    -7.308245696158815,
    3.60635441147954,
    -0.8461128860931261,
    0.10982698817978952,
)
COS_COEFFS = (
    1.4142134965649862,
    -6.978850988235484,
    5.7394611706121585,
    -1.8835629868567052,
    0.31069819092073886,
)

VMEM = pl.BlockSpec(memory_space=pltpu.VMEM)
SMEM = pl.BlockSpec(memory_space=pltpu.SMEM)


def horner(square, coeffs):
    total = square * coeffs[-1] + coeffs[-2]
    for coeff in coeffs[-3::-1]:
        total = total * square + coeff
    return total


def turn(cycles):
    part = cycles - jnp.round(cycles)
    square = part * part
    return part * horner(square, SIN_COEFFS), horner(square, COS_COEFFS)


def arrange_kernel(x_ref, o_ref):
    for panel_block in range(x_ref.shape[2] // LANES):
        for step in range(x_ref.shape[0]):
            o_ref[panel_block, step] = x_ref[step, :, panel_block * LANES : (panel_block + 1) * LANES]


def arrange(samples):
    steps, channels, panels = samples.shape
    chunk = 4096
    return pl.pallas_call(
        arrange_kernel,
        grid=(panels // chunk,),
        in_specs=[pl.BlockSpec((steps, channels, chunk), lambda i: (0, 0, i))],
        out_specs=pl.BlockSpec((chunk // LANES, steps, channels, LANES), lambda i: (i, 0, 0, 0)),
        out_shape=jax.ShapeDtypeStruct((panels // LANES, steps, channels, LANES), samples.dtype),
        name="arrange",
    )(samples)


def bins_of_block(bins_smem, b):
    row = lax.broadcasted_iota(jnp.int32, (8, LANES), 0) % 4
    bins = [jnp.full((8, LANES), bins_smem[4 * b + i], jnp.int32) for i in range(4)]
    chosen = jnp.where(row == 0, bins[0], jnp.where(row == 1, bins[1], jnp.where(row == 2, bins[2], bins[3])))
    return chosen.astype(jnp.float32)


def wave_copy(held_ref, waves_ref, sem, slot, rows, lanes):
    return pltpu.make_async_copy(held_ref.at[slot], waves_ref.at[:, :, rows, lanes], sem.at[slot])


def prepare_kernel(
    bins_smem,
    place_smem,
    obs_ref,
    panel_ref,
    waves_ref,
    inverse_ref,
    spread_ref,
    table_ref,
    pick_ref,
    column_ref,
    fine_ref,
    coarse_ref,
    held_ref,
    sem,
):
    start = pl.multiple_of(place_smem[0] * LANES, LANES)
    mine = panel_ref[:, pl.ds(start, LANES)]
    column_ref[...] = jnp.concatenate([mine, jnp.zeros((5, LANES), jnp.float32)], axis=0).T

    groups = obs_ref.shape[1] // LANES

    def one_tile(step, carry):
        row_tile, lane_tile, slot = step // groups, step % groups, step % 2
        rows = pl.ds(pl.multiple_of(row_tile * TILE, TILE), TILE)
        lanes = pl.ds(pl.multiple_of(lane_tile * LANES, LANES), LANES)
        offsets = [obs_ref[c : c + 1, lanes] - column_ref[rows, c : c + 1] for c in range(3)]
        square = offsets[0] * offsets[0] + offsets[1] * offsets[1] + offsets[2] * offsets[2]
        inverse = lax.rsqrt(square)
        inverse_ref[rows, lanes] = inverse
        cycles = square * inverse * (1.0 / (TIME * SPACING))

        sine, cosine = turn(cycles)
        sines, cosines = sine * cosine, 1.0 - sine * sine
        double = cosines + cosines
        fine = [(inverse, jnp.zeros_like(inverse)), (inverse * cosines, inverse * sines)]
        for n in range(2, 17):
            fine.append(tuple(double * fine[n - 1][i] - fine[n - 2][i] for i in range(2)))
        for n in range(17):
            fine_ref[16 + n, 0] = fine[n][0]
            fine_ref[16 + n, 1] = fine[n][1]
            if n:
                fine_ref[16 - n, 0] = fine[n][0]
                fine_ref[16 - n, 1] = -fine[n][1]

        sine, cosine = turn(cycles * 32.0)
        coarse = [(jnp.ones_like(inverse), jnp.zeros_like(inverse)), (1.0 - sine * sine, sine * cosine)]
        for n in range(1, 9):
            twice = coarse[n][0] + coarse[n][0]
            coarse.append((twice * coarse[n][0] - 1.0, twice * coarse[n][1]))
            if n < 8:
                coarse.append(
                    (twice * coarse[n + 1][0] - coarse[1][0], twice * coarse[n + 1][1] - coarse[1][1])
                )
        for n in range(17):
            coarse_ref[n, 0] = coarse[n][0]
            coarse_ref[n, 1] = coarse[n][1]

        @pl.when(step >= 2)
        def _():
            wave_copy(held_ref, waves_ref, sem, slot, 0, 0).wait()

        for j in range(NF):
            bin_number = bins_smem[j]
            whole = (bin_number + 16) >> 5
            rest = bin_number - (whole << 5) + 16
            c0, s0 = coarse_ref[whole, 0], coarse_ref[whole, 1]
            c1, s1 = fine_ref[rest, 0], fine_ref[rest, 1]
            held_ref[slot, j, 0] = c0 * c1 - s0 * s1
            held_ref[slot, j, 1] = s0 * c1 + c0 * s1
        wave_copy(held_ref, waves_ref, sem, slot, row_tile, lane_tile).start()
        return carry

    steps = (LANES // TILE) * groups
    lax.fori_loop(0, steps, one_tile, 0)

    obs = obs_ref[...]
    high = obs.astype(jnp.bfloat16).astype(jnp.float32)
    low = obs - high
    minus = jnp.full((6, obs.shape[1]), -1.0, jnp.float32)
    slot_rows = jnp.concatenate([high, high, low, minus, jnp.zeros((1, obs.shape[1]), jnp.float32)], axis=0)
    spread_ref[...] = jnp.zeros_like(spread_ref)
    for s in range(8):
        spread_ref[s, s * SLOT : (s + 1) * SLOT, :] = slot_rows.astype(jnp.bfloat16)

    rows = 2 * NF

    def one_chunk(chunk, carry):
        start = pl.multiple_of(chunk * LANES, LANES)
        column = lax.broadcasted_iota(jnp.int32, (8, LANES), 1) + start
        time = (column >> 2).astype(jnp.float32)
        channel = column & 3
        sine, cosine = turn(time * (1.0 / TIME))
        weight = (2.0 / TIME) * (0.5 * (sine * sine))
        is_real = lax.broadcasted_iota(jnp.int32, (8, LANES), 0) < 4
        values = []
        for b in range(BLOCKS):
            sine, cosine = turn(bins_of_block(bins_smem, b) * time * (1.0 / TIME))
            values.append(weight * jnp.where(is_real, 1.0 - sine * sine, -(sine * cosine)))
        values = jnp.concatenate(values, axis=0)
        channels = jnp.concatenate([channel] * BLOCKS, axis=0)
        for c in range(CHANNELS):
            table_ref[c * rows : (c + 1) * rows, pl.ds(start, LANES)] = jnp.where(
                channels == (c + 1) % CHANNELS, values, 0.0
            ).astype(jnp.bfloat16)
        return carry

    lax.fori_loop(0, TIME * CHANNELS // LANES, one_chunk, 0)

    source = lax.broadcasted_iota(jnp.int32, (rows, pick_ref.shape[1]), 0)
    target = lax.broadcasted_iota(jnp.int32, (rows, pick_ref.shape[1]), 1)
    same = jnp.where((target >> 4) == source, 1.0, 0.0)
    slot = lax.broadcasted_iota(jnp.int32, (8, pick_ref.shape[1]), 1) & 15
    for piece, bases in enumerate(((0, 6), (3, 3), (9, 9), (12, 12))):
        for direction in range(4):
            first = piece * 256 + direction * rows
            if direction == 3:
                pick_ref[first : first + rows, :] = jnp.zeros((rows, pick_ref.shape[1]), jnp.bfloat16)
                continue
            match = (slot == bases[0] + direction) | (slot == bases[1] + direction)
            chosen = jnp.where(match, 1.0, 0.0)
            pick_ref[first : first + rows, :] = (same * chosen[0:1]).astype(jnp.bfloat16)

    for step in (steps - 2, steps - 1):
        wave_copy(held_ref, waves_ref, sem, step % 2, 0, 0).wait()


def prepare(bins, place, obs, panel_position):
    observers = obs.shape[1]
    f32 = jnp.float32
    return pl.pallas_call(
        prepare_kernel,
        in_specs=[SMEM, SMEM, VMEM, VMEM],
        out_specs=[pl.BlockSpec(memory_space=pl.ANY)] + [VMEM] * 5,
        out_shape=[
            jax.ShapeDtypeStruct((NF, 2, LANES // TILE, observers // LANES, TILE, LANES), f32),
            jax.ShapeDtypeStruct((LANES, observers), f32),
            jax.ShapeDtypeStruct((8, LANES, observers), jnp.bfloat16),
            jax.ShapeDtypeStruct((CHANNELS * 2 * NF, CHANNELS * TIME), jnp.bfloat16),
            jax.ShapeDtypeStruct((1024, 1024), jnp.bfloat16),
            jax.ShapeDtypeStruct((LANES, 8), f32),
        ],
        scratch_shapes=[
            pltpu.VMEM((33, 2, TILE, LANES), f32),
            pltpu.VMEM((17, 2, TILE, LANES), f32),
            pltpu.VMEM((2, NF, 2, TILE, LANES), f32),
            pltpu.SemaphoreType.DMA((2,)),
        ],
        cost_estimate=pl.CostEstimate(flops=20_000_000_000, bytes_accessed=40_000_000, transcendentals=0),
        compiler_params=pltpu.CompilerParams(vmem_limit_bytes=32 << 20),
        name="prepare",
    )(bins, place, obs, panel_position)


def wave_fetch(waves_ref, held_ref, sem, j, slot):
    return pltpu.make_async_copy(waves_ref.at[j], held_ref.at[slot], sem.at[slot])


def radiate_kernel(
    bins_smem,
    data_ref,
    waves_ref,
    inverse_ref,
    spread_ref,
    table_ref,
    pick_ref,
    column_ref,
    scale_ref,
    o_ref,
    left_ref,
    mono_ref,
    product_ref,
    field_ref,
    held_ref,
    sem,
):
    for j in range(DEPTH):
        wave_fetch(waves_ref, held_ref, sem, j, j).start()
    spectra = jnp.dot(table_ref[...], data_ref[...], preferred_element_type=jnp.float32)
    scales = [
        bins_of_block(bins_smem, b) * (2.0 * math.pi / (TIME * SPACING)) * scale_ref[...] for b in range(BLOCKS)
    ]
    turned = (spectra * jnp.concatenate(scales * CHANNELS, axis=0)).T
    lane = lax.broadcasted_iota(jnp.int32, turned.shape, 1)
    position = jnp.where(
        lane < 64, column_ref[:, 0:1], jnp.where(lane < 128, column_ref[:, 1:2], column_ref[:, 2:3])
    )
    moment = turned * position
    high = turned.astype(jnp.bfloat16)
    low = (turned - high.astype(jnp.float32)).astype(jnp.bfloat16)
    moment_high = moment.astype(jnp.bfloat16)
    moment_low = (moment - moment_high.astype(jnp.float32)).astype(jnp.bfloat16)
    pieces = jnp.concatenate([high, low, moment_high, moment_low], axis=1)
    slots = jnp.dot(pieces, pick_ref[...], preferred_element_type=jnp.float32).astype(jnp.bfloat16)
    for b in range(BLOCKS):
        left_ref[b] = slots[:, b * LANES : (b + 1) * LANES]
        mono_ref[b, :, 0:8] = turned[:, 192 + 8 * b : 200 + 8 * b]

    panels = inverse_ref.shape[0]
    width = 256

    def one_block(b, carry):
        left = left_ref[b]
        for jj in range(4):
            j = b * 4 + jj
            held = (b % 2) * 4 + jj
            wave = jnp.full((8, LANES), bins_smem[j], jnp.int32).astype(jnp.float32)
            inverse_wave = 1.0 / (wave * (2.0 * math.pi / (TIME * SPACING)))
            mono_real = jnp.broadcast_to(mono_ref[b, :, jj : jj + 1], (panels, LANES))
            mono_imag = jnp.broadcast_to(mono_ref[b, :, 4 + jj : 5 + jj], (panels, LANES))
            wave_fetch(waves_ref, held_ref, sem, j, held).wait()
            for t in range(inverse_ref.shape[1] // width):
                parity = t % 2
                columns = slice(t * width, (t + 1) * width)
                product_ref[parity, 0] = jnp.dot(
                    left, spread_ref[jj, :, columns], preferred_element_type=jnp.float32
                )
                product_ref[parity, 1] = jnp.dot(
                    left, spread_ref[4 + jj, :, columns], preferred_element_type=jnp.float32
                )
                for half in range(2):
                    inner = slice(half * LANES, (half + 1) * LANES)
                    lane_tile = t * 2 + half
                    lanes = slice(lane_tile * LANES, (lane_tile + 1) * LANES)
                    sum_real = jnp.zeros((8, LANES), jnp.float32)
                    sum_imag = jnp.zeros((8, LANES), jnp.float32)
                    for p in range(panels // 8):
                        rows = slice(p * 8, p * 8 + 8)
                        row_tile, inside = p * 8 // TILE, slice(p * 8 % TILE, p * 8 % TILE + 8)
                        inverse = inverse_ref[rows, lanes]
                        cosine = held_ref[held, 0, row_tile, lane_tile, inside]
                        sine = held_ref[held, 1, row_tile, lane_tile, inside]
                        radial_real = product_ref[parity, 0, rows, inner] * inverse
                        radial_imag = product_ref[parity, 1, rows, inner] * inverse
                        near = inverse * inverse_wave
                        source_real = near * radial_real - (mono_imag[rows] + radial_imag)
                        source_imag = near * radial_imag + (mono_real[rows] + radial_real)
                        sum_real = sum_real + (cosine * source_real + sine * source_imag)
                        sum_imag = sum_imag + (cosine * source_imag - sine * source_real)
                    row = jj * 4 + t
                    field_ref[b, 0, row : row + 1, inner] = jnp.sum(sum_real, axis=0, keepdims=True)
                    field_ref[b, 1, row : row + 1, inner] = jnp.sum(sum_imag, axis=0, keepdims=True)

            @pl.when(j + DEPTH < NF)
            def _():
                wave_fetch(waves_ref, held_ref, sem, j + DEPTH, held).start()

        return carry

    lax.fori_loop(0, BLOCKS, one_block, 0)
    for part in range(2):
        flat = jnp.concatenate([field_ref[b, part] for b in range(BLOCKS)], axis=0)
        o_ref[:, part, :] = flat.T


def radiate(bins, data, prepared, scale):
    panels, observers = prepared[1].shape
    return pl.pallas_call(
        radiate_kernel,
        in_specs=[SMEM, VMEM, pl.BlockSpec(memory_space=pl.ANY)] + [VMEM] * 6,
        out_specs=VMEM,
        out_shape=jax.ShapeDtypeStruct((observers // 4, 2, LANES), jnp.float32),
        scratch_shapes=[
            pltpu.VMEM((BLOCKS, panels, LANES), jnp.bfloat16),
            pltpu.VMEM((BLOCKS, panels, LANES), jnp.float32),
            pltpu.VMEM((2, 2, panels, 256), jnp.float32),
            pltpu.VMEM((BLOCKS, 2, 16, 256), jnp.float32),
            pltpu.VMEM((DEPTH, 2, panels // TILE, observers // LANES, TILE, LANES), jnp.float32),
            pltpu.SemaphoreType.DMA((DEPTH,)),
        ],
        cost_estimate=pl.CostEstimate(flops=20_000_000_000, bytes_accessed=40_000_000, transcendentals=0),
        compiler_params=pltpu.CompilerParams(vmem_limit_bytes=40 << 20),
        name="radiate",
    )(bins, data, *prepared, scale)


def gather_kernel(x_ref, o_ref):
    total = jnp.sum(x_ref[...], axis=0)
    lane = lax.broadcasted_iota(jnp.int32, (NF, LANES), 1)
    row = lax.broadcasted_iota(jnp.int32, (NF, LANES), 0)
    for part in range(2):
        for i in range(4):
            o_ref[part, :, i : i + 1] = jnp.sum(
                jnp.where(lane == row * 4 + i, total[part : part + 1, :], 0.0), axis=1, keepdims=True
            )


def gather(arrived):
    return pl.pallas_call(
        gather_kernel,
        in_specs=[VMEM],
        out_specs=VMEM,
        out_shape=jax.ShapeDtypeStruct((2, NF, 4), jnp.float32),
        name="gather",
    )(arrived)


def all_observers(obs_position):
    whole = lax.all_gather(obs_position, "obs")
    whole = whole.reshape(lax.axis_size("obs"), 3, lax.axis_size("panel"), 4)
    return jnp.transpose(whole, (1, 3, 2, 0)).reshape(3, -1)


def local_field(data, place, panel_position, scale, observers, bins):
    prepared = prepare(bins, place, observers, panel_position)
    return radiate(bins, data, prepared, scale)


def shards(samples, panel_position, panel_area, panel_counts, obs_position, freq_bins):
    arrived = lax.all_to_all(arrange(samples), ("panel", "obs"), 0, 0, tiled=True)
    data = arrived.reshape(-1, LANES)

    place = lax.axis_index("obs")
    area = lax.dynamic_slice_in_dim(panel_area, place * LANES, LANES, 0)
    count = lax.dynamic_slice_in_dim(panel_counts, place, 1, 0)
    lane_ids = jnp.arange(LANES, dtype=jnp.int32)
    scale = jnp.where(lane_ids < count, area * (1.0 / (4.0 * math.pi)), 0.0)[None, :]

    observers = all_observers(obs_position)
    partial = local_field(data, place.reshape(1), panel_position, scale, observers, freq_bins)
    return gather(lax.all_to_all(partial, ("panel", "obs"), 0, 0, tiled=True))


def solution(mesh):
    in_specs = (
        P(("panel", "obs"), None, None),
        P(None, "panel"),
        P("panel"),
        P("panel"),
        P(None, "obs"),
        P(),
    )
    out_specs = P(None, None, ("obs", "panel"))
    return jax.shard_map(shards, mesh=mesh, in_specs=in_specs, out_specs=out_specs, check_vma=False)
```

```python
import math

import jax
import jax.numpy as jnp
from jax import lax
from jax.experimental import pallas as pl
from jax.experimental.pallas import tpu as pltpu
from jax.sharding import PartitionSpec as P


TIME = 1024
NF = 32
SPACING = 0.1
LANES = 128
CHANNELS = 4
AHEAD = 2
BLOCKS = 8
SLOTS = 4
TILE = 32
SLOT = 16

SIN_COEFFS = (
    4.442882919199695,
    -7.308245696158815,
    3.60635441147954,
    -0.8461128860931261,
    0.10982698817978952,
)
COS_COEFFS = (
    1.4142134965649862,
    -6.978850988235484,
    5.7394611706121585,
    -1.8835629868567052,
    0.31069819092073886,
)

VMEM = pl.BlockSpec(memory_space=pltpu.VMEM)
SMEM = pl.BlockSpec(memory_space=pltpu.SMEM)
HBM = pl.BlockSpec(memory_space=pltpu.HBM)


def horner(square, coeffs):
    total = square * coeffs[-1] + coeffs[-2]
    for coeff in coeffs[-3::-1]:
        total = total * square + coeff
    return total


def turn(cycles):
    part = cycles - jnp.round(cycles)
    square = part * part
    return part * horner(square, SIN_COEFFS), horner(square, COS_COEFFS)


def arrange_kernel(x_ref, o_ref, held_ref, sem):
    pieces, steps, _, piece = held_ref.shape
    copies = [
        pltpu.make_async_copy(x_ref.at[:, :, i * piece : (i + 1) * piece], held_ref.at[i], sem.at[i])
        for i in range(pieces)
    ]
    for copy in copies:
        copy.start()
    blocks = piece // LANES
    for i, copy in enumerate(copies):
        copy.wait()
        for block in range(blocks):
            for step in range(steps):
                o_ref[i * blocks + block, step] = held_ref[i, step, :, block * LANES : (block + 1) * LANES]


def arrange(samples):
    steps, channels, panels = samples.shape
    pieces = 4
    return pl.pallas_call(
        arrange_kernel,
        in_specs=[HBM],
        out_specs=VMEM,
        out_shape=jax.ShapeDtypeStruct((panels // LANES, steps, channels, LANES), samples.dtype),
        scratch_shapes=[
            pltpu.VMEM((pieces, steps, channels, panels // pieces), samples.dtype),
            pltpu.SemaphoreType.DMA((pieces,)),
        ],
        compiler_params=pltpu.CompilerParams(vmem_limit_bytes=8 << 20),
        name="arrange",
    )(pltpu.with_memory_space_constraint(samples, pltpu.HBM))


def bins_of_block(bins_smem, b):
    row = lax.broadcasted_iota(jnp.int32, (8, LANES), 0) % 4
    bins = [jnp.full((8, LANES), bins_smem[4 * b + i], jnp.int32) for i in range(4)]
    chosen = jnp.where(row == 0, bins[0], jnp.where(row == 1, bins[1], jnp.where(row == 2, bins[2], bins[3])))
    return chosen.astype(jnp.float32)


def wave_copy(held_ref, waves_ref, sem, slot, rows, lanes):
    return pltpu.make_async_copy(held_ref.at[slot], waves_ref.at[rows, lanes], sem.at[slot])


def prepare_kernel(
    bins_smem,
    place_smem,
    obs_ref,
    panel_ref,
    waves_ref,
    table_out_ref,
    column_ref,
    fine_ref,
    coarse_ref,
    held_ref,
    table_ref,
    sem,
    table_sem,
):
    start = pl.multiple_of(place_smem[0] * LANES, LANES)
    mine = panel_ref[:, pl.ds(start, LANES)]
    column_ref[...] = jnp.concatenate([mine, jnp.zeros((5, LANES), jnp.float32)], axis=0).T

    def one_chunk(chunk, carry):
        start = pl.multiple_of(chunk * LANES, LANES)
        time = ((lax.broadcasted_iota(jnp.int32, (8, LANES), 1) + start) >> 2).astype(jnp.float32)
        sine, cosine = turn(time * (1.0 / TIME))
        weight = (2.0 / TIME) * (0.5 * (sine * sine))
        is_real = lax.broadcasted_iota(jnp.int32, (8, LANES), 0) < 4
        values = []
        for b in range(BLOCKS):
            sine, cosine = turn(bins_of_block(bins_smem, b) * time * (1.0 / TIME))
            values.append(weight * jnp.where(is_real, 1.0 - sine * sine, -(sine * cosine)))
        table_ref[:, pl.ds(start, LANES)] = jnp.concatenate(values, axis=0).astype(jnp.bfloat16)
        return carry

    lax.fori_loop(0, TIME * CHANNELS // LANES, one_chunk, 0)
    table_copy = pltpu.make_async_copy(table_ref, table_out_ref, table_sem)
    table_copy.start()

    groups = obs_ref.shape[1] // LANES

    def one_tile(step, carry):
        row_tile, lane_tile, slot = step // groups, step % groups, step % SLOTS
        rows = pl.ds(pl.multiple_of(row_tile * TILE, TILE), TILE)
        lanes = pl.ds(pl.multiple_of(lane_tile * LANES, LANES), LANES)
        offsets = [obs_ref[c : c + 1, lanes] - column_ref[rows, c : c + 1] for c in range(3)]
        square = offsets[0] * offsets[0] + offsets[1] * offsets[1] + offsets[2] * offsets[2]
        inverse = lax.rsqrt(square)
        cycles = square * inverse * (1.0 / (TIME * SPACING))

        sine, cosine = turn(cycles)
        sines, cosines = sine * cosine, 1.0 - sine * sine
        double = cosines + cosines
        fine = [(inverse, jnp.zeros_like(inverse)), (inverse * cosines, inverse * sines)]
        for n in range(2, 17):
            fine.append(tuple(double * fine[n - 1][i] - fine[n - 2][i] for i in range(2)))
        for n in range(17):
            fine_ref[16 + n, 0] = fine[n][0]
            fine_ref[16 + n, 1] = fine[n][1]
            if n:
                fine_ref[16 - n, 0] = fine[n][0]
                fine_ref[16 - n, 1] = -fine[n][1]

        sine, cosine = turn(cycles * 32.0)
        coarse = [(jnp.ones_like(inverse), jnp.zeros_like(inverse)), (1.0 - sine * sine, sine * cosine)]
        for n in range(1, 9):
            twice = coarse[n][0] + coarse[n][0]
            coarse.append((twice * coarse[n][0] - 1.0, twice * coarse[n][1]))
            if n < 8:
                coarse.append(
                    (twice * coarse[n + 1][0] - coarse[1][0], twice * coarse[n + 1][1] - coarse[1][1])
                )
        for n in range(17):
            coarse_ref[n, 0] = coarse[n][0]
            coarse_ref[n, 1] = coarse[n][1]

        @pl.when(step >= SLOTS)
        def _():
            wave_copy(held_ref, waves_ref, sem, slot, 0, 0).wait()

        for j in range(NF):
            bin_number = bins_smem[j]
            whole = (bin_number + 16) >> 5
            rest = bin_number - (whole << 5) + 16
            c0, s0 = coarse_ref[whole, 0], coarse_ref[whole, 1]
            c1, s1 = fine_ref[rest, 0], fine_ref[rest, 1]
            held_ref[slot, j, 0] = (c0 * c1 - s0 * s1).astype(jnp.bfloat16)
            held_ref[slot, j, 1] = (s0 * c1 + c0 * s1).astype(jnp.bfloat16)
        wave_copy(held_ref, waves_ref, sem, slot, row_tile, lane_tile).start()
        return carry

    steps = (LANES // TILE) * groups
    lax.fori_loop(0, steps, one_tile, 0)

    for slot in range(SLOTS):
        wave_copy(held_ref, waves_ref, sem, slot, 0, 0).wait()
    table_copy.wait()


def prepare(bins, place, obs, panel_position):
    observers = obs.shape[1]
    f32 = jnp.float32
    return pl.pallas_call(
        prepare_kernel,
        in_specs=[SMEM, SMEM, VMEM, VMEM],
        out_specs=[HBM] * 2 + [VMEM],
        out_shape=[
            pltpu.HBM((LANES // TILE, observers // LANES, NF, 2, TILE, LANES), jnp.bfloat16),
            pltpu.HBM((2 * NF, CHANNELS * TIME), jnp.bfloat16),
            jax.ShapeDtypeStruct((LANES, 8), f32),
        ],
        scratch_shapes=[
            pltpu.VMEM((33, 2, TILE, LANES), f32),
            pltpu.VMEM((17, 2, TILE, LANES), f32),
            pltpu.VMEM((SLOTS, NF, 2, TILE, LANES), jnp.bfloat16),
            pltpu.VMEM((2 * NF, CHANNELS * TIME), jnp.bfloat16),
            pltpu.SemaphoreType.DMA((SLOTS,)),
            pltpu.SemaphoreType.DMA,
        ],
        cost_estimate=pl.CostEstimate(flops=20_000_000_000, bytes_accessed=40_000_000, transcendentals=0),
        compiler_params=pltpu.CompilerParams(vmem_limit_bytes=16 << 20),
        name="prepare",
    )(bins, place, obs, panel_position)


def wave_fetch(waves_ref, held_ref, sem, b):
    return pltpu.make_async_copy(waves_ref.at[:, :, pl.ds(b * 4, 4)], held_ref.at[b], sem.at[b])


def radiate_kernel(
    bins_smem,
    data_ref,
    obs_ref,
    waves_ref,
    table_in_ref,
    column_ref,
    scale_ref,
    o_ref,
    left_ref,
    mono_ref,
    product_ref,
    field_ref,
    inverse_ref,
    spread_ref,
    pick_ref,
    narrow_ref,
    table_ref,
    held_ref,
    sem,
    table_sem,
):
    table_copy = pltpu.make_async_copy(table_in_ref, narrow_ref, table_sem)
    table_copy.start()
    rows = 2 * NF

    obs = obs_ref[...]
    high = obs.astype(jnp.bfloat16).astype(jnp.float32)
    low = obs - high
    minus = jnp.full((6, obs.shape[1]), -1.0, jnp.float32)
    slot_rows = jnp.concatenate([high, high, low, minus, jnp.zeros((1, obs.shape[1]), jnp.float32)], axis=0)
    spread_ref[...] = jnp.zeros_like(spread_ref)
    for s in range(8):
        spread_ref[s, s * SLOT : (s + 1) * SLOT, :] = slot_rows.astype(jnp.bfloat16)

    for group in range(obs_ref.shape[1] // LANES):
        lanes = slice(group * LANES, (group + 1) * LANES)
        offsets = [obs_ref[c : c + 1, lanes] - column_ref[:, c : c + 1] for c in range(3)]
        square = offsets[0] * offsets[0] + offsets[1] * offsets[1] + offsets[2] * offsets[2]
        inverse_ref[:, lanes] = lax.rsqrt(square)

    source = lax.broadcasted_iota(jnp.int32, (rows, pick_ref.shape[1]), 0)
    target = lax.broadcasted_iota(jnp.int32, (rows, pick_ref.shape[1]), 1)
    same = jnp.where((target >> 4) == source, 1.0, 0.0)
    slot = lax.broadcasted_iota(jnp.int32, (8, pick_ref.shape[1]), 1) & 15
    for piece, bases in enumerate(((0, 6), (3, 3), (9, 9), (12, 12))):
        for direction in range(4):
            first = piece * 256 + direction * rows
            if direction == 3:
                pick_ref[first : first + rows, :] = jnp.zeros((rows, pick_ref.shape[1]), jnp.bfloat16)
                continue
            match = (slot == bases[0] + direction) | (slot == bases[1] + direction)
            chosen = jnp.where(match, 1.0, 0.0)
            pick_ref[first : first + rows, :] = (same * chosen[0:1]).astype(jnp.bfloat16)

    channel = lax.broadcasted_iota(jnp.int32, (16, LANES), 1) & 3
    table_copy.wait()
    for b in range(AHEAD):
        wave_fetch(waves_ref, held_ref, sem, b).start()
    for c in range(CHANNELS):
        mask = jnp.where(channel == (c + 1) % CHANNELS, 1.0, 0.0).astype(jnp.bfloat16)[0:1]
        for chunk in range(CHANNELS * TIME // LANES):
            lanes = slice(chunk * LANES, (chunk + 1) * LANES)
            table_ref[c * rows : (c + 1) * rows, lanes] = narrow_ref[:, lanes] * mask
    spectra = jnp.dot(table_ref[...], data_ref[...], preferred_element_type=jnp.float32)
    scales = [
        bins_of_block(bins_smem, b) * (2.0 * math.pi / (TIME * SPACING)) * scale_ref[...] for b in range(BLOCKS)
    ]
    turned = (spectra * jnp.concatenate(scales * CHANNELS, axis=0)).T
    lane = lax.broadcasted_iota(jnp.int32, turned.shape, 1)
    position = jnp.where(
        lane < 64, column_ref[:, 0:1], jnp.where(lane < 128, column_ref[:, 1:2], column_ref[:, 2:3])
    )
    moment = turned * position
    high = turned.astype(jnp.bfloat16)
    low = (turned - high.astype(jnp.float32)).astype(jnp.bfloat16)
    moment_high = moment.astype(jnp.bfloat16)
    moment_low = (moment - moment_high.astype(jnp.float32)).astype(jnp.bfloat16)
    pieces = jnp.concatenate([high, low, moment_high, moment_low], axis=1)
    slots = jnp.dot(pieces, pick_ref[...], preferred_element_type=jnp.float32).astype(jnp.bfloat16)
    for b in range(BLOCKS):
        left_ref[b] = slots[:, b * LANES : (b + 1) * LANES]
        mono_ref[b, :, 0:8] = turned[:, 192 + 8 * b : 200 + 8 * b]

    panels = inverse_ref.shape[0]
    width = 256

    def one_block(b, carry):
        @pl.when(b + AHEAD < BLOCKS)
        def _():
            wave_fetch(waves_ref, held_ref, sem, b + AHEAD).start()

        left = left_ref[b]
        wave_fetch(waves_ref, held_ref, sem, b).wait()
        for jj in range(4):
            j = b * 4 + jj
            wave = jnp.full((8, LANES), bins_smem[j], jnp.int32).astype(jnp.float32)
            inverse_wave = 1.0 / (wave * (2.0 * math.pi / (TIME * SPACING)))
            mono_real = jnp.broadcast_to(mono_ref[b, :, jj : jj + 1], (panels, LANES))
            mono_imag = jnp.broadcast_to(mono_ref[b, :, 4 + jj : 5 + jj], (panels, LANES))
            for t in range(inverse_ref.shape[1] // width):
                parity = t % 2
                columns = slice(t * width, (t + 1) * width)
                product_ref[parity, 0] = jnp.dot(
                    left, spread_ref[jj, :, columns], preferred_element_type=jnp.float32
                )
                product_ref[parity, 1] = jnp.dot(
                    left, spread_ref[4 + jj, :, columns], preferred_element_type=jnp.float32
                )
                for half in range(2):
                    inner = slice(half * LANES, (half + 1) * LANES)
                    lane_tile = t * 2 + half
                    lanes = slice(lane_tile * LANES, (lane_tile + 1) * LANES)
                    sum_real = jnp.zeros((8, LANES), jnp.float32)
                    sum_imag = jnp.zeros((8, LANES), jnp.float32)
                    for p in range(panels // 8):
                        rows = slice(p * 8, p * 8 + 8)
                        inverse = inverse_ref[rows, lanes]
                        if p % 2 == 0:
                            row_tile, inside = p * 8 // TILE, slice(p * 8 % TILE, p * 8 % TILE + 16)
                            cosines = held_ref[b, row_tile, lane_tile, jj, 0, inside].astype(jnp.float32)
                            sines = held_ref[b, row_tile, lane_tile, jj, 1, inside].astype(jnp.float32)
                        cosine = cosines[p % 2 * 8 : p % 2 * 8 + 8]
                        sine = sines[p % 2 * 8 : p % 2 * 8 + 8]
                        radial_real = product_ref[parity, 0, rows, inner] * inverse
                        radial_imag = product_ref[parity, 1, rows, inner] * inverse
                        near = inverse * inverse_wave
                        source_real = near * radial_real - (mono_imag[rows] + radial_imag)
                        source_imag = near * radial_imag + (mono_real[rows] + radial_real)
                        sum_real = sum_real + (cosine * source_real + sine * source_imag)
                        sum_imag = sum_imag + (cosine * source_imag - sine * source_real)
                    row = t * 4 + jj
                    field_ref[b, 0, row : row + 1, inner] = jnp.sum(sum_real, axis=0, keepdims=True)
                    field_ref[b, 1, row : row + 1, inner] = jnp.sum(sum_imag, axis=0, keepdims=True)
        return carry

    lax.fori_loop(0, BLOCKS, one_block, 0)
    for part in range(2):
        flat = jnp.concatenate(
            [field_ref[b, part, 4 * t : 4 * t + 4] for t in range(4) for b in range(BLOCKS)], axis=0
        )
        o_ref[:, part, :] = flat.T


def radiate(bins, data, observers, prepared, scale):
    panels, count = LANES, observers.shape[1]
    return pl.pallas_call(
        radiate_kernel,
        in_specs=[SMEM, VMEM, VMEM, HBM, HBM, VMEM, VMEM],
        out_specs=VMEM,
        out_shape=jax.ShapeDtypeStruct((count // 4, 2, LANES), jnp.float32),
        scratch_shapes=[
            pltpu.VMEM((BLOCKS, panels, LANES), jnp.bfloat16),
            pltpu.VMEM((BLOCKS, panels, LANES), jnp.float32),
            pltpu.VMEM((2, 2, panels, 256), jnp.float32),
            pltpu.VMEM((BLOCKS, 2, 16, 256), jnp.float32),
            pltpu.VMEM((panels, count), jnp.float32),
            pltpu.VMEM((8, LANES, count), jnp.bfloat16),
            pltpu.VMEM((1024, 1024), jnp.bfloat16),
            pltpu.VMEM((2 * NF, CHANNELS * TIME), jnp.bfloat16),
            pltpu.VMEM((CHANNELS * 2 * NF, CHANNELS * TIME), jnp.bfloat16),
            pltpu.VMEM((BLOCKS, panels // TILE, count // LANES, 4, 2, TILE, LANES), jnp.bfloat16),
            pltpu.SemaphoreType.DMA((BLOCKS,)),
            pltpu.SemaphoreType.DMA,
        ],
        cost_estimate=pl.CostEstimate(flops=20_000_000_000, bytes_accessed=40_000_000, transcendentals=0),
        compiler_params=pltpu.CompilerParams(vmem_limit_bytes=40 << 20),
        name="radiate",
    )(bins, data, observers, *prepared, scale)


def gather_kernel(x_ref, o_ref):
    total = jnp.sum(x_ref[...], axis=0)
    for part in range(2):
        for i in range(4):
            o_ref[part, i : i + 1, :] = total[part : part + 1, i * NF : (i + 1) * NF]


def gather(arrived):
    return pl.pallas_call(
        gather_kernel,
        in_specs=[VMEM],
        out_specs=VMEM,
        out_shape=jax.ShapeDtypeStruct((2, 4, NF), jnp.float32),
        name="gather",
    )(arrived)


def all_observers(obs_position):
    size = lax.axis_size("obs")
    local = jnp.transpose(obs_position.reshape(3, -1, 4), (0, 2, 1)).reshape(12, -1)
    held = [local]
    for shift in range(1, size):
        held.append(lax.ppermute(local, "obs", [((i + shift) % size, i) for i in range(size)]))
    own = lax.axis_index("obs")
    ring = jnp.stack(held + held)
    whole = lax.dynamic_slice_in_dim(ring, (size - own) % size, size, 0)
    return jnp.transpose(whole, (1, 2, 0)).reshape(3, -1)


def local_field(data, place, panel_position, scale, observers, bins):
    prepared = prepare(bins, place, observers, panel_position)
    waves, table, columns = prepared
    held = [pltpu.with_memory_space_constraint(v, pltpu.HBM) for v in (waves, table)]
    return radiate(bins, data, observers, (*held, columns), scale)


def shards(samples, panel_position, panel_area, panel_counts, obs_position, freq_bins):
    arrived = lax.all_to_all(arrange(samples), ("panel", "obs"), 0, 0, tiled=True)
    data = arrived.reshape(-1, LANES)
    observers = all_observers(obs_position)

    place = lax.axis_index("obs")
    area = lax.dynamic_slice_in_dim(panel_area, place * LANES, LANES, 0)
    count = lax.dynamic_slice_in_dim(panel_counts, place, 1, 0)
    lane_ids = jnp.arange(LANES, dtype=jnp.int32)
    scale = jnp.where(lane_ids < count, area * (1.0 / (4.0 * math.pi)), 0.0)[None, :]

    partial = local_field(data, place.reshape(1), panel_position, scale, observers, freq_bins)
    arrived = lax.all_to_all(partial, ("panel", "obs"), 0, 0, tiled=True)
    return jnp.transpose(gather(arrived), (0, 2, 1))


def solution(mesh):
    in_specs = (
        P(("panel", "obs"), None, None),
        P(None, "panel"),
        P("panel"),
        P("panel"),
        P(None, "obs"),
        P(),
    )
    out_specs = P(None, None, ("obs", "panel"))
    return jax.shard_map(shards, mesh=mesh, in_specs=in_specs, out_specs=out_specs, check_vma=False)
```

```python
import math

import jax
import jax.numpy as jnp
from jax import lax
from jax.experimental import pallas as pl
from jax.experimental.pallas import tpu as pltpu
from jax.sharding import PartitionSpec as P


TIME = 1024
NF = 32
SPACING = 0.1
LANES = 128
CHANNELS = 4
AHEAD = 3
BLOCKS = 8
SLOTS = 4
TILE = 32

SIN_COEFFS = (
    4.442882919199695,
    -7.308245696158815,
    3.60635441147954,
    -0.8461128860931261,
    0.10982698817978952,
)
COS_COEFFS = (
    1.4142134965649862,
    -6.978850988235484,
    5.7394611706121585,
    -1.8835629868567052,
    0.31069819092073886,
)

VMEM = pl.BlockSpec(memory_space=pltpu.VMEM)
SMEM = pl.BlockSpec(memory_space=pltpu.SMEM)
HBM = pl.BlockSpec(memory_space=pltpu.HBM)


def horner(square, coeffs):
    total = square * coeffs[-1] + coeffs[-2]
    for coeff in coeffs[-3::-1]:
        total = total * square + coeff
    return total


def turn(cycles):
    part = cycles - jnp.round(cycles)
    square = part * part
    return part * horner(square, SIN_COEFFS), horner(square, COS_COEFFS)


def arrange_kernel(x_ref, o_ref, held_ref, sem):
    pieces, steps, _, piece = held_ref.shape
    copies = [
        pltpu.make_async_copy(x_ref.at[:, :, i * piece : (i + 1) * piece], held_ref.at[i], sem.at[i])
        for i in range(pieces)
    ]
    for copy in copies:
        copy.start()
    blocks = piece // LANES
    for i, copy in enumerate(copies):
        copy.wait()
        for block in range(blocks):
            for step in range(steps):
                o_ref[i * blocks + block, step] = held_ref[i, step, :, block * LANES : (block + 1) * LANES]


def arrange(samples):
    steps, channels, panels = samples.shape
    pieces = 4
    return pl.pallas_call(
        arrange_kernel,
        in_specs=[HBM],
        out_specs=VMEM,
        out_shape=jax.ShapeDtypeStruct((panels // LANES, steps, channels, LANES), samples.dtype),
        scratch_shapes=[
            pltpu.VMEM((pieces, steps, channels, panels // pieces), samples.dtype),
            pltpu.SemaphoreType.DMA((pieces,)),
        ],
        compiler_params=pltpu.CompilerParams(vmem_limit_bytes=8 << 20),
        name="arrange",
    )(pltpu.with_memory_space_constraint(samples, pltpu.HBM))


def bins_of_block(bins_smem, b):
    row = lax.broadcasted_iota(jnp.int32, (8, LANES), 0) % 4
    bins = [jnp.full((8, LANES), bins_smem[4 * b + i], jnp.int32) for i in range(4)]
    chosen = jnp.where(row == 0, bins[0], jnp.where(row == 1, bins[1], jnp.where(row == 2, bins[2], bins[3])))
    return chosen.astype(jnp.float32)


def wave_copy(held_ref, waves_ref, sem, slot, rows, lanes):
    return pltpu.make_async_copy(held_ref.at[slot], waves_ref.at[rows, lanes], sem.at[slot])


def prepare_kernel(
    bins_smem,
    place_smem,
    obs_ref,
    panel_ref,
    waves_ref,
    table_out_ref,
    column_ref,
    position_ref,
    fine_ref,
    coarse_ref,
    held_ref,
    table_ref,
    sem,
    table_sem,
):
    start = pl.multiple_of(place_smem[0] * LANES, LANES)
    mine = panel_ref[:, pl.ds(start, LANES)]
    position_ref[...] = jnp.concatenate([mine, jnp.zeros((5, LANES), jnp.float32)], axis=0)
    column_ref[...] = position_ref[...].T

    def one_chunk(chunk, carry):
        start = pl.multiple_of(chunk * LANES, LANES)
        time = ((lax.broadcasted_iota(jnp.int32, (8, LANES), 1) + start) >> 2).astype(jnp.float32)
        sine, cosine = turn(time * (1.0 / TIME))
        weight = (2.0 / TIME) * (0.5 * (sine * sine))
        is_real = lax.broadcasted_iota(jnp.int32, (8, LANES), 0) < 4
        values = []
        for b in range(BLOCKS):
            sine, cosine = turn(bins_of_block(bins_smem, b) * time * (1.0 / TIME))
            values.append(weight * jnp.where(is_real, 1.0 - sine * sine, -(sine * cosine)))
        table_ref[:, pl.ds(start, LANES)] = jnp.concatenate(values, axis=0).astype(jnp.bfloat16)
        return carry

    lax.fori_loop(0, TIME * CHANNELS // LANES, one_chunk, 0)
    table_copy = pltpu.make_async_copy(table_ref, table_out_ref, table_sem)
    table_copy.start()

    groups = obs_ref.shape[1] // LANES

    def one_tile(step, carry):
        row_tile, lane_tile, slot = step // groups, step % groups, step % SLOTS
        rows = pl.ds(pl.multiple_of(row_tile * TILE, TILE), TILE)
        lanes = pl.ds(pl.multiple_of(lane_tile * LANES, LANES), LANES)
        offsets = [obs_ref[c : c + 1, lanes] - column_ref[rows, c : c + 1] for c in range(3)]
        square = offsets[0] * offsets[0] + offsets[1] * offsets[1] + offsets[2] * offsets[2]
        inverse = lax.rsqrt(square)
        cycles = square * inverse * (1.0 / (TIME * SPACING))

        sine, cosine = turn(cycles)
        sines, cosines = sine * cosine, 1.0 - sine * sine
        double = cosines + cosines
        fine = [(inverse, jnp.zeros_like(inverse)), (inverse * cosines, inverse * sines)]
        for n in range(2, 17):
            fine.append(tuple(double * fine[n - 1][i] - fine[n - 2][i] for i in range(2)))
        for n in range(17):
            fine_ref[16 + n, 0] = fine[n][0]
            fine_ref[16 + n, 1] = fine[n][1]
            if n:
                fine_ref[16 - n, 0] = fine[n][0]
                fine_ref[16 - n, 1] = -fine[n][1]

        sine, cosine = turn(cycles * 32.0)
        coarse = [(jnp.ones_like(inverse), jnp.zeros_like(inverse)), (1.0 - sine * sine, sine * cosine)]
        for n in range(1, 9):
            twice = coarse[n][0] + coarse[n][0]
            coarse.append((twice * coarse[n][0] - 1.0, twice * coarse[n][1]))
            if n < 8:
                coarse.append(
                    (twice * coarse[n + 1][0] - coarse[1][0], twice * coarse[n + 1][1] - coarse[1][1])
                )
        for n in range(17):
            coarse_ref[n, 0] = coarse[n][0]
            coarse_ref[n, 1] = coarse[n][1]

        @pl.when(step >= SLOTS)
        def _():
            wave_copy(held_ref, waves_ref, sem, slot, 0, 0).wait()

        for j in range(NF):
            bin_number = bins_smem[j]
            whole = (bin_number + 16) >> 5
            rest = bin_number - (whole << 5) + 16
            c0, s0 = coarse_ref[whole, 0], coarse_ref[whole, 1]
            c1, s1 = fine_ref[rest, 0], fine_ref[rest, 1]
            held_ref[slot, j, 0] = (c0 * c1 - s0 * s1).astype(jnp.bfloat16)
            held_ref[slot, j, 1] = (s0 * c1 + c0 * s1).astype(jnp.bfloat16)
        wave_copy(held_ref, waves_ref, sem, slot, row_tile, lane_tile).start()
        return carry

    steps = (LANES // TILE) * groups
    lax.fori_loop(0, steps, one_tile, 0)

    for slot in range(SLOTS):
        wave_copy(held_ref, waves_ref, sem, slot, 0, 0).wait()
    table_copy.wait()


def prepare(bins, place, obs, panel_position):
    observers = obs.shape[1]
    f32 = jnp.float32
    return pl.pallas_call(
        prepare_kernel,
        in_specs=[SMEM, SMEM, VMEM, VMEM],
        out_specs=[HBM] * 2 + [VMEM] * 2,
        out_shape=[
            pltpu.HBM((LANES // TILE, observers // LANES, NF, 2, TILE, LANES), jnp.bfloat16),
            pltpu.HBM((2 * NF, CHANNELS * TIME), jnp.bfloat16),
            jax.ShapeDtypeStruct((LANES, 8), f32),
            jax.ShapeDtypeStruct((8, LANES), f32),
        ],
        scratch_shapes=[
            pltpu.VMEM((33, 2, TILE, LANES), f32),
            pltpu.VMEM((17, 2, TILE, LANES), f32),
            pltpu.VMEM((SLOTS, NF, 2, TILE, LANES), jnp.bfloat16),
            pltpu.VMEM((2 * NF, CHANNELS * TIME), jnp.bfloat16),
            pltpu.SemaphoreType.DMA((SLOTS,)),
            pltpu.SemaphoreType.DMA,
        ],
        cost_estimate=pl.CostEstimate(flops=20_000_000_000, bytes_accessed=40_000_000, transcendentals=0),
        compiler_params=pltpu.CompilerParams(vmem_limit_bytes=16 << 20),
        name="prepare",
    )(bins, place, obs, panel_position)


def wave_fetch(waves_ref, held_ref, sem, b):
    return pltpu.make_async_copy(waves_ref.at[:, :, pl.ds(b * 4, 4)], held_ref.at[b], sem.at[b])


def radiate_kernel(
    bins_smem,
    data_in_ref,
    obs_ref,
    waves_ref,
    table_in_ref,
    column_ref,
    position_ref,
    scale_ref,
    o_ref,
    left_ref,
    product_ref,
    field_ref,
    inverse_ref,
    spread_ref,
    narrow_ref,
    table_ref,
    data_ref,
    source_ref,
    held_ref,
    sem,
    in_sem,
):
    table_copy = pltpu.make_async_copy(table_in_ref, narrow_ref, in_sem.at[0])
    table_copy.start()
    data_copy = pltpu.make_async_copy(data_in_ref, data_ref, in_sem.at[1])
    data_copy.start()
    for b in range(AHEAD):
        wave_fetch(waves_ref, held_ref, sem, b).start()
    rows = 2 * NF

    obs = obs_ref[...]
    high = obs.astype(jnp.bfloat16).astype(jnp.float32)
    low = obs - high
    minus = jnp.full((1, obs.shape[1]), -1.0, jnp.float32)
    factors = [v[c : c + 1] for v in (high, high, low) for c in range(3)] + [minus] * 6 + [minus * 0.0]
    spread_ref[...] = jnp.concatenate(
        [jnp.broadcast_to(v, (8, obs.shape[1])) for v in factors], axis=0
    ).astype(jnp.bfloat16)
    for group in range(obs_ref.shape[1] // LANES):
        lanes = slice(group * LANES, (group + 1) * LANES)
        offsets = [obs_ref[c : c + 1, lanes] - column_ref[:, c : c + 1] for c in range(3)]
        square = offsets[0] * offsets[0] + offsets[1] * offsets[1] + offsets[2] * offsets[2]
        inverse_ref[:, lanes] = lax.rsqrt(square)

    channel = lax.broadcasted_iota(jnp.int32, (16, LANES), 1) & 3
    table_copy.wait()
    for c in range(CHANNELS):
        mask = jnp.where(channel == (c + 1) % CHANNELS, 1.0, 0.0).astype(jnp.bfloat16)[0:1]
        for chunk in range(CHANNELS * TIME // LANES):
            lanes = slice(chunk * LANES, (chunk + 1) * LANES)
            table_ref[c * rows : (c + 1) * rows, lanes] = narrow_ref[:, lanes] * mask
    data_copy.wait()
    spectra = jnp.dot(table_ref[...], data_ref[...], preferred_element_type=jnp.float32)
    scales = [
        bins_of_block(bins_smem, b) * (2.0 * math.pi / (TIME * SPACING)) * scale_ref[...] for b in range(BLOCKS)
    ]
    spectra = spectra * jnp.concatenate(scales * CHANNELS, axis=0)
    row = lax.broadcasted_iota(jnp.int32, (8, LANES), 0)
    blank = jnp.zeros((8, 2 * LANES), jnp.float32)
    for b in range(BLOCKS):
        whole = spectra[192 + 8 * b : 200 + 8 * b]
        lead = whole.astype(jnp.bfloat16).astype(jnp.float32)
        rest = whole - lead
        for jj in range(4):
            real = jnp.where(row < 2, lead[jj : jj + 1], rest[jj : jj + 1])
            imag = jnp.where(row < 2, lead[4 + jj : 5 + jj], rest[4 + jj : 5 + jj])
            by_cosine = jnp.where(row % 2 == 0, -imag, real)
            by_sine = jnp.where(row % 2 == 0, real, imag)
            both = jnp.where(lax.broadcasted_iota(jnp.int32, (8, 2 * LANES), 0) < 4, jnp.concatenate([by_cosine, by_sine], axis=1), 0.0)
            source_ref[4 * b + jj] = jnp.concatenate([both, blank], axis=0).astype(jnp.bfloat16)
    for b in range(BLOCKS):
        direct = [spectra[c * rows + 8 * b : c * rows + 8 * b + 8] for c in range(3)]
        moment = [direct[c] * position_ref[c : c + 1, :] for c in range(3)]
        lead = [v.astype(jnp.bfloat16).astype(jnp.float32) for v in direct + moment]
        rest = [v - w for v, w in zip(direct + moment, lead)]
        slots = lead[:3] + rest[:3] + lead[:3] + lead[3:] + rest[3:] + [jnp.zeros((8, LANES), jnp.float32)]
        left_ref[b] = jnp.concatenate(slots, axis=0).T.astype(jnp.bfloat16)

    panels = inverse_ref.shape[0]
    width = 256

    def one_block(b, carry):
        @pl.when(b + AHEAD < BLOCKS)
        def _():
            wave_fetch(waves_ref, held_ref, sem, b + AHEAD).start()

        left = left_ref[b]
        lane = lax.broadcasted_iota(jnp.int32, (16, LANES), 1) & 7
        wave_fetch(waves_ref, held_ref, sem, b).wait()
        for jj in range(4):
            j = b * 4 + jj
            wave = jnp.full((8, LANES), bins_smem[j], jnp.int32).astype(jnp.float32)
            inverse_wave = 1.0 / (wave * (2.0 * math.pi / (TIME * SPACING)))
            source = source_ref[j]
            parts = [
                left * jnp.where(lane == s, 1.0, 0.0).astype(jnp.bfloat16)[0:1] for s in (jj, 4 + jj)
            ]
            for t in range(inverse_ref.shape[1] // width):
                parity = t % 2
                columns = slice(t * width, (t + 1) * width)
                for part in range(2):
                    product_ref[parity, part] = jnp.dot(
                        parts[part], spread_ref[:, columns], preferred_element_type=jnp.float32
                    )
                weights = jnp.concatenate(
                    [
                        jnp.concatenate([held_ref[b, i, 2 * t + half, jj, part] for half in range(2)], axis=1)
                        for part in range(2)
                        for i in range(panels // TILE)
                    ],
                    axis=0,
                )
                mono = jnp.dot(source, weights, preferred_element_type=jnp.float32)
                for half in range(2):
                    inner = slice(half * LANES, (half + 1) * LANES)
                    lane_tile = t * 2 + half
                    lanes = slice(lane_tile * LANES, (lane_tile + 1) * LANES)
                    far_real = far_imag = near_real = near_imag = jnp.zeros((8, LANES), jnp.float32)
                    for p in range(panels // 8):
                        rows = slice(p * 8, p * 8 + 8)
                        inverse = inverse_ref[rows, lanes]
                        if p % 2 == 0:
                            row_tile, inside = p * 8 // TILE, slice(p * 8 % TILE, p * 8 % TILE + 16)
                            cosines = held_ref[b, row_tile, lane_tile, jj, 0, inside].astype(jnp.float32)
                            sines = held_ref[b, row_tile, lane_tile, jj, 1, inside].astype(jnp.float32)
                        cosine = cosines[p % 2 * 8 : p % 2 * 8 + 8]
                        sine = sines[p % 2 * 8 : p % 2 * 8 + 8]
                        radial_real = product_ref[parity, 0, rows, inner] * inverse
                        radial_imag = product_ref[parity, 1, rows, inner] * inverse
                        term_real = cosine * radial_real + sine * radial_imag
                        term_imag = cosine * radial_imag - sine * radial_real
                        far_real = far_real + term_real
                        far_imag = far_imag + term_imag
                        near_real = near_real + inverse * term_real
                        near_imag = near_imag + inverse * term_imag
                    row = t * 4 + jj
                    sum_real = jnp.sum(near_real * inverse_wave - far_imag, axis=0, keepdims=True)
                    sum_imag = jnp.sum(near_imag * inverse_wave + far_real, axis=0, keepdims=True)
                    field_ref[b, 0, row : row + 1, inner] = sum_real + (mono[0:1, inner] + mono[2:3, inner])
                    field_ref[b, 1, row : row + 1, inner] = sum_imag + (mono[1:2, inner] + mono[3:4, inner])
        return carry

    lax.fori_loop(0, BLOCKS, one_block, 0)
    for part in range(2):
        flat = jnp.concatenate(
            [field_ref[b, part, 4 * t : 4 * t + 4] for t in range(4) for b in range(BLOCKS)], axis=0
        )
        o_ref[:, part, :] = flat.T


def radiate(bins, data, observers, prepared, scale):
    panels, count = LANES, observers.shape[1]
    return pl.pallas_call(
        radiate_kernel,
        in_specs=[SMEM, pl.BlockSpec(memory_space=pl.ANY), VMEM, HBM, HBM, VMEM, VMEM, VMEM],
        out_specs=VMEM,
        out_shape=jax.ShapeDtypeStruct((count // 4, 2, LANES), jnp.float32),
        scratch_shapes=[
            pltpu.VMEM((BLOCKS, panels, LANES), jnp.bfloat16),
            pltpu.VMEM((2, 2, panels, 256), jnp.float32),
            pltpu.VMEM((BLOCKS, 2, 16, 256), jnp.float32),
            pltpu.VMEM((panels, count), jnp.float32),
            pltpu.VMEM((LANES, count), jnp.bfloat16),
            pltpu.VMEM((2 * NF, CHANNELS * TIME), jnp.bfloat16),
            pltpu.VMEM((CHANNELS * 2 * NF, CHANNELS * TIME), jnp.bfloat16),
            pltpu.VMEM((CHANNELS * TIME, LANES), jnp.bfloat16),
            pltpu.VMEM((NF, 16, 2 * LANES), jnp.bfloat16),
            pltpu.VMEM((BLOCKS, panels // TILE, count // LANES, 4, 2, TILE, LANES), jnp.bfloat16),
            pltpu.SemaphoreType.DMA((BLOCKS,)),
            pltpu.SemaphoreType.DMA((2,)),
        ],
        cost_estimate=pl.CostEstimate(flops=20_000_000_000, bytes_accessed=40_000_000, transcendentals=0),
        compiler_params=pltpu.CompilerParams(vmem_limit_bytes=40 << 20),
        name="radiate",
    )(bins, data, observers, *prepared, scale)


def gather_kernel(x_ref, o_ref):
    total = jnp.sum(x_ref[...], axis=0)
    for part in range(2):
        for i in range(4):
            o_ref[part, i : i + 1, :] = total[part : part + 1, i * NF : (i + 1) * NF]


def gather(arrived):
    return pl.pallas_call(
        gather_kernel,
        in_specs=[VMEM],
        out_specs=VMEM,
        out_shape=jax.ShapeDtypeStruct((2, 4, NF), jnp.float32),
        name="gather",
    )(arrived)


def all_observers(obs_position):
    size = lax.axis_size("obs")
    local = jnp.transpose(obs_position.reshape(3, -1, 4), (0, 2, 1)).reshape(12, -1)
    held = [local]
    for shift in range(1, size):
        held.append(lax.ppermute(local, "obs", [((i + shift) % size, i) for i in range(size)]))
    own = lax.axis_index("obs")
    ring = jnp.stack(held + held)
    whole = lax.dynamic_slice_in_dim(ring, (size - own) % size, size, 0)
    return jnp.transpose(whole, (1, 2, 0)).reshape(3, -1)


def local_field(data, place, panel_position, scale, observers, bins):
    prepared = prepare(bins, place, observers, panel_position)
    waves, table, columns, position = prepared
    held = [pltpu.with_memory_space_constraint(v, pltpu.HBM) for v in (waves, table)]
    return radiate(bins, data, observers, (*held, columns, position), scale)


def shards(samples, panel_position, panel_area, panel_counts, obs_position, freq_bins):
    arrived = lax.all_to_all(arrange(samples), ("panel", "obs"), 0, 0, tiled=True)
    data = arrived.reshape(-1, LANES)
    observers = all_observers(obs_position)

    place = lax.axis_index("obs")
    area = lax.dynamic_slice_in_dim(panel_area, place * LANES, LANES, 0)
    count = lax.dynamic_slice_in_dim(panel_counts, place, 1, 0)
    lane_ids = jnp.arange(LANES, dtype=jnp.int32)
    scale = jnp.where(lane_ids < count, area * (1.0 / (4.0 * math.pi)), 0.0)[None, :]

    partial = local_field(data, place.reshape(1), panel_position, scale, observers, freq_bins)
    arrived = lax.all_to_all(partial, ("panel", "obs"), 0, 0, tiled=True)
    return jnp.transpose(gather(arrived), (0, 2, 1))


def solution(mesh):
    in_specs = (
        P(("panel", "obs"), None, None),
        P(None, "panel"),
        P("panel"),
        P("panel"),
        P(None, "obs"),
        P(),
    )
    out_specs = P(None, None, ("obs", "panel"))
    return jax.shard_map(shards, mesh=mesh, in_specs=in_specs, out_specs=out_specs, check_vma=False)
```

```python
import math

import jax
import jax.numpy as jnp
from jax import lax
from jax.experimental import pallas as pl
from jax.experimental.pallas import tpu as pltpu
from jax.sharding import PartitionSpec as P


TIME = 1024
NF = 32
SPACING = 0.1
LANES = 128
CHANNELS = 4
AHEAD = 3
BLOCKS = 8
SLOTS = 4
TILE = 32

SIN_COEFFS = (
    4.442882919199695,
    -7.308245696158815,
    3.60635441147954,
    -0.8461128860931261,
    0.10982698817978952,
)
COS_COEFFS = (
    1.4142134965649862,
    -6.978850988235484,
    5.7394611706121585,
    -1.8835629868567052,
    0.31069819092073886,
)

VMEM = pl.BlockSpec(memory_space=pltpu.VMEM)
SMEM = pl.BlockSpec(memory_space=pltpu.SMEM)
HBM = pl.BlockSpec(memory_space=pltpu.HBM)


def horner(square, coeffs):
    total = square * coeffs[-1] + coeffs[-2]
    for coeff in coeffs[-3::-1]:
        total = total * square + coeff
    return total


def turn(cycles):
    part = cycles - jnp.round(cycles)
    square = part * part
    return part * horner(square, SIN_COEFFS), horner(square, COS_COEFFS)


def arrange_kernel(x_ref, o_ref, held_ref, made_ref, sem, out_sem):
    pieces, steps, _, piece = held_ref.shape
    copies = [
        pltpu.make_async_copy(x_ref.at[:, :, i * piece : (i + 1) * piece], held_ref.at[i], sem.at[i])
        for i in range(pieces)
    ]
    for copy in copies:
        copy.start()
    blocks = piece // LANES

    def outward(i):
        done = pl.ds(i * blocks, blocks)
        return pltpu.make_async_copy(made_ref.at[done], o_ref.at[done], out_sem.at[i])

    for i, copy in enumerate(copies):
        copy.wait()
        for block in range(blocks):
            for step in range(steps):
                made_ref[i * blocks + block, step] = held_ref[i, step, :, block * LANES : (block + 1) * LANES]
        outward(i).start()
    for i in range(pieces):
        outward(i).wait()


def arrange(samples):
    steps, channels, panels = samples.shape
    pieces = 4
    return pl.pallas_call(
        arrange_kernel,
        in_specs=[HBM],
        out_specs=HBM,
        out_shape=pltpu.HBM((panels // LANES, steps, channels, LANES), samples.dtype),
        scratch_shapes=[
            pltpu.VMEM((pieces, steps, channels, panels // pieces), samples.dtype),
            pltpu.VMEM((panels // LANES, steps, channels, LANES), samples.dtype),
            pltpu.SemaphoreType.DMA((pieces,)),
            pltpu.SemaphoreType.DMA((pieces,)),
        ],
        compiler_params=pltpu.CompilerParams(vmem_limit_bytes=8 << 20),
        name="arrange",
    )(pltpu.with_memory_space_constraint(samples, pltpu.HBM))


def bins_of_block(bins_smem, b):
    row = lax.broadcasted_iota(jnp.int32, (8, LANES), 0) % 4
    bins = [jnp.full((8, LANES), bins_smem[4 * b + i], jnp.int32) for i in range(4)]
    chosen = jnp.where(row == 0, bins[0], jnp.where(row == 1, bins[1], jnp.where(row == 2, bins[2], bins[3])))
    return chosen.astype(jnp.float32)


def wave_copy(held_ref, waves_ref, sem, slot, rows, lanes):
    return pltpu.make_async_copy(held_ref.at[slot], waves_ref.at[rows, lanes], sem.at[slot])


def prepare_kernel(
    bins_smem,
    place_smem,
    obs_ref,
    panel_ref,
    waves_ref,
    table_out_ref,
    column_ref,
    position_ref,
    fine_ref,
    coarse_ref,
    held_ref,
    table_ref,
    sem,
    table_sem,
):
    start = pl.multiple_of(place_smem[0] * LANES, LANES)
    mine = panel_ref[:, pl.ds(start, LANES)]
    position_ref[...] = jnp.concatenate([mine, jnp.zeros((5, LANES), jnp.float32)], axis=0)
    column_ref[...] = position_ref[...].T

    def one_chunk(chunk, carry):
        start = pl.multiple_of(chunk * LANES, LANES)
        time = ((lax.broadcasted_iota(jnp.int32, (8, LANES), 1) + start) >> 2).astype(jnp.float32)
        sine, cosine = turn(time * (1.0 / TIME))
        weight = (2.0 / TIME) * (0.5 * (sine * sine))
        is_real = lax.broadcasted_iota(jnp.int32, (8, LANES), 0) < 4
        values = []
        for b in range(BLOCKS):
            sine, cosine = turn(bins_of_block(bins_smem, b) * time * (1.0 / TIME))
            values.append(weight * jnp.where(is_real, 1.0 - sine * sine, -(sine * cosine)))
        table_ref[:, pl.ds(start, LANES)] = jnp.concatenate(values, axis=0).astype(jnp.bfloat16)
        return carry

    lax.fori_loop(0, TIME * CHANNELS // LANES, one_chunk, 0)
    table_copy = pltpu.make_async_copy(table_ref, table_out_ref, table_sem)
    table_copy.start()

    groups = obs_ref.shape[1] // LANES

    def one_tile(step, carry):
        row_tile, lane_tile, slot = step // groups, step % groups, step % SLOTS
        rows = pl.ds(pl.multiple_of(row_tile * TILE, TILE), TILE)
        lanes = pl.ds(pl.multiple_of(lane_tile * LANES, LANES), LANES)
        offsets = [obs_ref[c : c + 1, lanes] - column_ref[rows, c : c + 1] for c in range(3)]
        square = offsets[0] * offsets[0] + offsets[1] * offsets[1] + offsets[2] * offsets[2]
        inverse = lax.rsqrt(square)
        cycles = square * inverse * (1.0 / (TIME * SPACING))

        sine, cosine = turn(cycles)
        sines, cosines = sine * cosine, 1.0 - sine * sine
        double = cosines + cosines
        fine = [(inverse, jnp.zeros_like(inverse)), (inverse * cosines, inverse * sines)]
        for n in range(2, 17):
            fine.append(tuple(double * fine[n - 1][i] - fine[n - 2][i] for i in range(2)))
        for n in range(17):
            fine_ref[16 + n, 0] = fine[n][0]
            fine_ref[16 + n, 1] = fine[n][1]
            if n:
                fine_ref[16 - n, 0] = fine[n][0]
                fine_ref[16 - n, 1] = -fine[n][1]

        sine, cosine = turn(cycles * 32.0)
        coarse = [(jnp.ones_like(inverse), jnp.zeros_like(inverse)), (1.0 - sine * sine, sine * cosine)]
        for n in range(1, 9):
            twice = coarse[n][0] + coarse[n][0]
            coarse.append((twice * coarse[n][0] - 1.0, twice * coarse[n][1]))
            if n < 8:
                coarse.append(
                    (twice * coarse[n + 1][0] - coarse[1][0], twice * coarse[n + 1][1] - coarse[1][1])
                )
        for n in range(17):
            coarse_ref[n, 0] = coarse[n][0]
            coarse_ref[n, 1] = coarse[n][1]

        @pl.when(step >= SLOTS)
        def _():
            wave_copy(held_ref, waves_ref, sem, slot, 0, 0).wait()

        for j in range(NF):
            bin_number = bins_smem[j]
            whole = (bin_number + 16) >> 5
            rest = bin_number - (whole << 5) + 16
            c0, s0 = coarse_ref[whole, 0], coarse_ref[whole, 1]
            c1, s1 = fine_ref[rest, 0], fine_ref[rest, 1]
            held_ref[slot, j, 0] = (c0 * c1 - s0 * s1).astype(jnp.bfloat16)
            held_ref[slot, j, 1] = (s0 * c1 + c0 * s1).astype(jnp.bfloat16)
        wave_copy(held_ref, waves_ref, sem, slot, row_tile, lane_tile).start()
        return carry

    steps = (LANES // TILE) * groups
    lax.fori_loop(0, steps, one_tile, 0)

    for slot in range(SLOTS):
        wave_copy(held_ref, waves_ref, sem, slot, 0, 0).wait()
    table_copy.wait()


def prepare(bins, place, obs, panel_position):
    observers = obs.shape[1]
    f32 = jnp.float32
    return pl.pallas_call(
        prepare_kernel,
        in_specs=[SMEM, SMEM, VMEM, VMEM],
        out_specs=[HBM] * 2 + [VMEM] * 2,
        out_shape=[
            pltpu.HBM((LANES // TILE, observers // LANES, NF, 2, TILE, LANES), jnp.bfloat16),
            pltpu.HBM((2 * NF, CHANNELS * TIME), jnp.bfloat16),
            jax.ShapeDtypeStruct((LANES, 8), f32),
            jax.ShapeDtypeStruct((8, LANES), f32),
        ],
        scratch_shapes=[
            pltpu.VMEM((33, 2, TILE, LANES), f32),
            pltpu.VMEM((17, 2, TILE, LANES), f32),
            pltpu.VMEM((SLOTS, NF, 2, TILE, LANES), jnp.bfloat16),
            pltpu.VMEM((2 * NF, CHANNELS * TIME), jnp.bfloat16),
            pltpu.SemaphoreType.DMA((SLOTS,)),
            pltpu.SemaphoreType.DMA,
        ],
        cost_estimate=pl.CostEstimate(flops=20_000_000_000, bytes_accessed=40_000_000, transcendentals=0),
        compiler_params=pltpu.CompilerParams(vmem_limit_bytes=16 << 20),
        name="prepare",
    )(bins, place, obs, panel_position)


def wave_fetch(waves_ref, held_ref, sem, b):
    return pltpu.make_async_copy(waves_ref.at[:, :, pl.ds(b * 4, 4)], held_ref.at[b], sem.at[b])


def radiate_kernel(
    bins_smem,
    data_in_ref,
    obs_in_ref,
    waves_ref,
    table_in_ref,
    column_in_ref,
    position_in_ref,
    scale_in_ref,
    o_ref,
    left_ref,
    product_ref,
    field_ref,
    inverse_ref,
    spread_ref,
    narrow_ref,
    table_ref,
    data_ref,
    source_ref,
    held_ref,
    obs_ref,
    column_ref,
    position_ref,
    scale_ref,
    made_ref,
    sem,
    in_sem,
    out_sem,
):
    small = [
        pltpu.make_async_copy(source, target, in_sem.at[2 + i])
        for i, (source, target) in enumerate(
            (
                (obs_in_ref, obs_ref),
                (column_in_ref, column_ref),
                (position_in_ref, position_ref),
                (scale_in_ref, scale_ref),
            )
        )
    ]
    for copy in small:
        copy.start()
    table_copy = pltpu.make_async_copy(table_in_ref, narrow_ref, in_sem.at[0])
    table_copy.start()
    data_copy = pltpu.make_async_copy(data_in_ref, data_ref, in_sem.at[1])
    data_copy.start()
    for b in range(AHEAD):
        wave_fetch(waves_ref, held_ref, sem, b).start()
    rows = 2 * NF

    for copy in small:
        copy.wait()

    obs = obs_ref[...]
    high = obs.astype(jnp.bfloat16).astype(jnp.float32)
    low = obs - high
    minus = jnp.full((1, obs.shape[1]), -1.0, jnp.float32)
    factors = [v[c : c + 1] for v in (high, high, low) for c in range(3)] + [minus] * 6 + [minus * 0.0]
    spread_ref[...] = jnp.concatenate(
        [jnp.broadcast_to(v, (8, obs.shape[1])) for v in factors], axis=0
    ).astype(jnp.bfloat16)
    for group in range(obs_ref.shape[1] // LANES):
        lanes = slice(group * LANES, (group + 1) * LANES)
        offsets = [obs_ref[c : c + 1, lanes] - column_ref[:, c : c + 1] for c in range(3)]
        square = offsets[0] * offsets[0] + offsets[1] * offsets[1] + offsets[2] * offsets[2]
        inverse_ref[:, lanes] = lax.rsqrt(square)

    channel = lax.broadcasted_iota(jnp.int32, (16, LANES), 1) & 3
    table_copy.wait()
    for c in range(CHANNELS):
        mask = jnp.where(channel == (c + 1) % CHANNELS, 1.0, 0.0).astype(jnp.bfloat16)[0:1]
        for chunk in range(CHANNELS * TIME // LANES):
            lanes = slice(chunk * LANES, (chunk + 1) * LANES)
            table_ref[c * rows : (c + 1) * rows, lanes] = narrow_ref[:, lanes] * mask
    data_copy.wait()
    spectra = jnp.dot(table_ref[...], data_ref[...], preferred_element_type=jnp.float32)
    scales = [
        bins_of_block(bins_smem, b) * (2.0 * math.pi / (TIME * SPACING)) * scale_ref[...] for b in range(BLOCKS)
    ]
    spectra = spectra * jnp.concatenate(scales * CHANNELS, axis=0)
    row = lax.broadcasted_iota(jnp.int32, (8, LANES), 0)
    blank = jnp.zeros((8, 2 * LANES), jnp.float32)
    for b in range(BLOCKS):
        whole = spectra[192 + 8 * b : 200 + 8 * b]
        lead = whole.astype(jnp.bfloat16).astype(jnp.float32)
        rest = whole - lead
        for jj in range(4):
            real = jnp.where(row < 2, lead[jj : jj + 1], rest[jj : jj + 1])
            imag = jnp.where(row < 2, lead[4 + jj : 5 + jj], rest[4 + jj : 5 + jj])
            by_cosine = jnp.where(row % 2 == 0, -imag, real)
            by_sine = jnp.where(row % 2 == 0, real, imag)
            both = jnp.where(lax.broadcasted_iota(jnp.int32, (8, 2 * LANES), 0) < 4, jnp.concatenate([by_cosine, by_sine], axis=1), 0.0)
            source_ref[4 * b + jj] = jnp.concatenate([both, blank], axis=0).astype(jnp.bfloat16)
    for b in range(BLOCKS):
        direct = [spectra[c * rows + 8 * b : c * rows + 8 * b + 8] for c in range(3)]
        moment = [direct[c] * position_ref[c : c + 1, :] for c in range(3)]
        lead = [v.astype(jnp.bfloat16).astype(jnp.float32) for v in direct + moment]
        rest = [v - w for v, w in zip(direct + moment, lead)]
        slots = lead[:3] + rest[:3] + lead[:3] + lead[3:] + rest[3:] + [jnp.zeros((8, LANES), jnp.float32)]
        left_ref[b] = jnp.concatenate(slots, axis=0).T.astype(jnp.bfloat16)

    panels = inverse_ref.shape[0]
    width = 256

    def one_block(b, carry):
        @pl.when(b + AHEAD < BLOCKS)
        def _():
            wave_fetch(waves_ref, held_ref, sem, b + AHEAD).start()

        left = left_ref[b]
        lane = lax.broadcasted_iota(jnp.int32, (16, LANES), 1) & 7
        wave_fetch(waves_ref, held_ref, sem, b).wait()
        for jj in range(4):
            j = b * 4 + jj
            wave = jnp.full((8, LANES), bins_smem[j], jnp.int32).astype(jnp.float32)
            inverse_wave = 1.0 / (wave * (2.0 * math.pi / (TIME * SPACING)))
            source = source_ref[j]
            parts = [
                left * jnp.where(lane == s, 1.0, 0.0).astype(jnp.bfloat16)[0:1] for s in (jj, 4 + jj)
            ]
            for t in range(inverse_ref.shape[1] // width):
                parity = t % 2
                columns = slice(t * width, (t + 1) * width)
                for part in range(2):
                    product_ref[parity, part] = jnp.dot(
                        parts[part], spread_ref[:, columns], preferred_element_type=jnp.float32
                    )
                weights = jnp.concatenate(
                    [
                        jnp.concatenate([held_ref[b, i, 2 * t + half, jj, part] for half in range(2)], axis=1)
                        for part in range(2)
                        for i in range(panels // TILE)
                    ],
                    axis=0,
                )
                mono = jnp.dot(source, weights, preferred_element_type=jnp.float32)
                for half in range(2):
                    inner = slice(half * LANES, (half + 1) * LANES)
                    lane_tile = t * 2 + half
                    lanes = slice(lane_tile * LANES, (lane_tile + 1) * LANES)
                    far_real = far_imag = near_real = near_imag = jnp.zeros((8, LANES), jnp.float32)
                    for p in range(panels // 8):
                        rows = slice(p * 8, p * 8 + 8)
                        inverse = inverse_ref[rows, lanes]
                        if p % 2 == 0:
                            row_tile, inside = p * 8 // TILE, slice(p * 8 % TILE, p * 8 % TILE + 16)
                            cosines = held_ref[b, row_tile, lane_tile, jj, 0, inside].astype(jnp.float32)
                            sines = held_ref[b, row_tile, lane_tile, jj, 1, inside].astype(jnp.float32)
                        cosine = cosines[p % 2 * 8 : p % 2 * 8 + 8]
                        sine = sines[p % 2 * 8 : p % 2 * 8 + 8]
                        radial_real = product_ref[parity, 0, rows, inner] * inverse
                        radial_imag = product_ref[parity, 1, rows, inner] * inverse
                        term_real = cosine * radial_real + sine * radial_imag
                        term_imag = cosine * radial_imag - sine * radial_real
                        far_real = far_real + term_real
                        far_imag = far_imag + term_imag
                        near_real = near_real + inverse * term_real
                        near_imag = near_imag + inverse * term_imag
                    row = t * 4 + jj
                    sum_real = jnp.sum(near_real * inverse_wave - far_imag, axis=0, keepdims=True)
                    sum_imag = jnp.sum(near_imag * inverse_wave + far_real, axis=0, keepdims=True)
                    field_ref[b, 0, row : row + 1, inner] = sum_real + (mono[0:1, inner] + mono[2:3, inner])
                    field_ref[b, 1, row : row + 1, inner] = sum_imag + (mono[1:2, inner] + mono[3:4, inner])
        return carry

    lax.fori_loop(0, BLOCKS, one_block, 0)
    copies = []
    for half in range(2):
        lanes = slice(half * LANES, (half + 1) * LANES)
        for part in range(2):
            flat = jnp.concatenate(
                [field_ref[b, part, 4 * t : 4 * t + 4, lanes] for t in range(4) for b in range(BLOCKS)], axis=0
            )
            made_ref[pl.ds(half * 2 * LANES + part, LANES, 2), :] = flat.T
        done = pl.ds(half * 2 * LANES, 2 * LANES)
        copies.append(pltpu.make_async_copy(made_ref.at[done], o_ref.at[done], out_sem.at[half]))
        copies[half].start()
    for copy in copies:
        copy.wait()


def radiate(bins, data, observers, prepared, scale):
    panels, count = LANES, observers.shape[1]
    anywhere = pl.BlockSpec(memory_space=pl.ANY)
    return pl.pallas_call(
        radiate_kernel,
        in_specs=[SMEM, anywhere, anywhere, HBM, HBM, anywhere, anywhere, anywhere],
        out_specs=HBM,
        out_shape=pltpu.HBM((count // 2, LANES), jnp.float32),
        scratch_shapes=[
            pltpu.VMEM((BLOCKS, panels, LANES), jnp.bfloat16),
            pltpu.VMEM((2, 2, panels, 256), jnp.float32),
            pltpu.VMEM((BLOCKS, 2, 16, 256), jnp.float32),
            pltpu.VMEM((panels, count), jnp.float32),
            pltpu.VMEM((LANES, count), jnp.bfloat16),
            pltpu.VMEM((2 * NF, CHANNELS * TIME), jnp.bfloat16),
            pltpu.VMEM((CHANNELS * 2 * NF, CHANNELS * TIME), jnp.bfloat16),
            pltpu.VMEM((CHANNELS * TIME, LANES), jnp.bfloat16),
            pltpu.VMEM((NF, 16, 2 * LANES), jnp.bfloat16),
            pltpu.VMEM((BLOCKS, panels // TILE, count // LANES, 4, 2, TILE, LANES), jnp.bfloat16),
            pltpu.VMEM((3, count), jnp.float32),
            pltpu.VMEM((panels, 8), jnp.float32),
            pltpu.VMEM((8, panels), jnp.float32),
            pltpu.VMEM((1, panels), jnp.float32),
            pltpu.VMEM((count // 2, LANES), jnp.float32),
            pltpu.SemaphoreType.DMA((BLOCKS,)),
            pltpu.SemaphoreType.DMA((6,)),
            pltpu.SemaphoreType.DMA((2,)),
        ],
        cost_estimate=pl.CostEstimate(flops=20_000_000_000, bytes_accessed=40_000_000, transcendentals=0),
        compiler_params=pltpu.CompilerParams(vmem_limit_bytes=40 << 20),
        name="radiate",
    )(bins, data, observers, *prepared, scale)


def gather_kernel(x_ref, o_ref):
    total = jnp.zeros((8, LANES), jnp.float32)
    sums = [total, total, total, total]
    for i in range(x_ref.shape[0] // 8):
        sums[i % 4] = sums[i % 4] + x_ref[8 * i : 8 * i + 8, :]
    total = (sums[0] + sums[1]) + (sums[2] + sums[3])
    for part in range(2):
        whole = (total[part : part + 1] + total[part + 2 : part + 3]) + (
            total[part + 4 : part + 5] + total[part + 6 : part + 7]
        )
        for i in range(4):
            o_ref[part, i : i + 1, :] = whole[:, i * NF : (i + 1) * NF]


def gather(arrived):
    return pl.pallas_call(
        gather_kernel,
        in_specs=[VMEM],
        out_specs=VMEM,
        out_shape=jax.ShapeDtypeStruct((2, 4, NF), jnp.float32),
        name="gather",
    )(arrived)


def all_observers(obs_position):
    size = lax.axis_size("obs")
    local = jnp.transpose(obs_position.reshape(3, -1, 4), (0, 2, 1)).reshape(12, -1)
    held = [local]
    for shift in range(1, size):
        held.append(lax.ppermute(local, "obs", [((i + shift) % size, i) for i in range(size)]))
    own = lax.axis_index("obs")
    ring = jnp.stack(held + held)
    whole = lax.dynamic_slice_in_dim(ring, (size - own) % size, size, 0)
    return jnp.transpose(whole, (1, 2, 0)).reshape(3, -1)


def local_field(data, place, panel_position, scale, observers, bins):
    prepared = prepare(bins, place, observers, panel_position)
    waves, table, columns, position = prepared
    held = [pltpu.with_memory_space_constraint(v, pltpu.HBM) for v in (waves, table)]
    return radiate(bins, data, observers, (*held, columns, position), scale)


def shards(samples, panel_position, panel_area, panel_counts, obs_position, freq_bins):
    arrived = lax.all_to_all(arrange(samples), ("panel", "obs"), 0, 0, tiled=True)
    data = arrived.reshape(-1, LANES)
    observers = all_observers(obs_position)

    place = lax.axis_index("obs")
    area = lax.dynamic_slice_in_dim(panel_area, place * LANES, LANES, 0)
    count = lax.dynamic_slice_in_dim(panel_counts, place, 1, 0)
    lane_ids = jnp.arange(LANES, dtype=jnp.int32)
    scale = jnp.where(lane_ids < count, area * (1.0 / (4.0 * math.pi)), 0.0)[None, :]

    partial = local_field(data, place.reshape(1), panel_position, scale, observers, freq_bins)
    partial = partial.reshape(-1, 2, LANES)
    arrived = lax.all_to_all(partial, ("panel", "obs"), 0, 0, tiled=True)
    arrived = arrived.reshape(-1, LANES)
    return jnp.transpose(gather(arrived), (0, 2, 1))


def solution(mesh):
    in_specs = (
        P(("panel", "obs"), None, None),
        P(None, "panel"),
        P("panel"),
        P("panel"),
        P(None, "obs"),
        P(),
    )
    out_specs = P(None, None, ("obs", "panel"))
    return jax.shard_map(shards, mesh=mesh, in_specs=in_specs, out_specs=out_specs, check_vma=False)
```

```python
import math

import jax
import jax.numpy as jnp
from jax import lax
from jax.experimental import pallas as pl
from jax.experimental.pallas import tpu as pltpu
from jax.sharding import PartitionSpec as P


TIME = 1024
NF = 32
SPACING = 0.1
LANES = 128
CHANNELS = 4
AHEAD = 3
BLOCKS = 8
SLOTS = 4
TILE = 32

SIN_COEFFS = (
    4.442882919199695,
    -7.308245696158815,
    3.60635441147954,
    -0.8461128860931261,
    0.10982698817978952,
)
COS_COEFFS = (
    1.4142134965649862,
    -6.978850988235484,
    5.7394611706121585,
    -1.8835629868567052,
    0.31069819092073886,
)

VMEM = pl.BlockSpec(memory_space=pltpu.VMEM)
SMEM = pl.BlockSpec(memory_space=pltpu.SMEM)
HBM = pl.BlockSpec(memory_space=pltpu.HBM)


def horner(square, coeffs):
    total = square * coeffs[-1] + coeffs[-2]
    for coeff in coeffs[-3::-1]:
        total = total * square + coeff
    return total


def turn(cycles):
    part = cycles - jnp.round(cycles)
    square = part * part
    return part * horner(square, SIN_COEFFS), horner(square, COS_COEFFS)


def arrange_kernel(x_ref, o_ref, held_ref, made_ref, sem, out_sem):
    pieces, steps, _, piece = held_ref.shape
    copies = [
        pltpu.make_async_copy(x_ref.at[:, :, i * piece : (i + 1) * piece], held_ref.at[i], sem.at[i])
        for i in range(pieces)
    ]
    for copy in copies:
        copy.start()
    blocks = piece // LANES

    def outward(i):
        done = pl.ds(i * blocks, blocks)
        return pltpu.make_async_copy(made_ref.at[done], o_ref.at[done], out_sem.at[i])

    for i, copy in enumerate(copies):
        copy.wait()
        for block in range(blocks):
            for step in range(steps):
                made_ref[i * blocks + block, step] = held_ref[i, step, :, block * LANES : (block + 1) * LANES]
        outward(i).start()
    for i in range(pieces):
        outward(i).wait()


def arrange(samples):
    steps, channels, panels = samples.shape
    pieces = 4
    return pl.pallas_call(
        arrange_kernel,
        in_specs=[HBM],
        out_specs=HBM,
        out_shape=pltpu.HBM((panels // LANES, steps, channels, LANES), samples.dtype),
        scratch_shapes=[
            pltpu.VMEM((pieces, steps, channels, panels // pieces), samples.dtype),
            pltpu.VMEM((panels // LANES, steps, channels, LANES), samples.dtype),
            pltpu.SemaphoreType.DMA((pieces,)),
            pltpu.SemaphoreType.DMA((pieces,)),
        ],
        compiler_params=pltpu.CompilerParams(vmem_limit_bytes=8 << 20),
        name="arrange",
    )(pltpu.with_memory_space_constraint(samples, pltpu.HBM))


def bins_of_block(bins_smem, b):
    row = lax.broadcasted_iota(jnp.int32, (8, LANES), 0) % 4
    bins = [jnp.full((8, LANES), bins_smem[4 * b + i], jnp.int32) for i in range(4)]
    chosen = jnp.where(row == 0, bins[0], jnp.where(row == 1, bins[1], jnp.where(row == 2, bins[2], bins[3])))
    return chosen.astype(jnp.float32)


def wave_copy(held_ref, waves_ref, sem, slot, rows, lanes):
    return pltpu.make_async_copy(held_ref.at[slot], waves_ref.at[rows, lanes], sem.at[slot])


def prepare_kernel(
    bins_smem,
    place_smem,
    counts_smem,
    area_in_ref,
    obs_ref,
    panel_in_ref,
    waves_ref,
    table_out_ref,
    column_ref,
    position_ref,
    scale_ref,
    fine_ref,
    coarse_ref,
    held_ref,
    table_ref,
    sem,
    table_sem,
    area_ref,
    panel_ref,
    small_sem,
):
    small = [
        pltpu.make_async_copy(area_in_ref, area_ref, small_sem.at[0]),
        pltpu.make_async_copy(panel_in_ref, panel_ref, small_sem.at[1]),
    ]
    for copy in small:
        copy.start()
    for copy in small:
        copy.wait()
    start = pl.multiple_of(place_smem[0] * LANES, LANES)
    mine = panel_ref[:, pl.ds(start, LANES)]
    position_ref[...] = jnp.concatenate([mine, jnp.zeros((5, LANES), jnp.float32)], axis=0)
    column_ref[...] = position_ref[...].T
    area = area_ref[0:1]
    for i in range(1, area_ref.shape[0]):
        area = jnp.where(place_smem[0] == i, area_ref[i : i + 1], area)
    live = lax.broadcasted_iota(jnp.int32, (1, LANES), 1) < counts_smem[place_smem[0]]
    scale_ref[...] = jnp.where(live, area * (1.0 / (4.0 * math.pi)), 0.0)

    def one_chunk(chunk, carry):
        start = pl.multiple_of(chunk * LANES, LANES)
        time = ((lax.broadcasted_iota(jnp.int32, (8, LANES), 1) + start) >> 2).astype(jnp.float32)
        sine, cosine = turn(time * (1.0 / TIME))
        weight = (2.0 / TIME) * (0.5 * (sine * sine))
        is_real = lax.broadcasted_iota(jnp.int32, (8, LANES), 0) < 4
        values = []
        for b in range(BLOCKS):
            sine, cosine = turn(bins_of_block(bins_smem, b) * time * (1.0 / TIME))
            values.append(weight * jnp.where(is_real, 1.0 - sine * sine, -(sine * cosine)))
        table_ref[:, pl.ds(start, LANES)] = jnp.concatenate(values, axis=0).astype(jnp.bfloat16)
        return carry

    lax.fori_loop(0, TIME * CHANNELS // LANES, one_chunk, 0)
    table_copy = pltpu.make_async_copy(table_ref, table_out_ref, table_sem)
    table_copy.start()

    groups = obs_ref.shape[1] // LANES

    def one_tile(step, carry):
        row_tile, lane_tile, slot = step // groups, step % groups, step % SLOTS
        rows = pl.ds(pl.multiple_of(row_tile * TILE, TILE), TILE)
        lanes = pl.ds(pl.multiple_of(lane_tile * LANES, LANES), LANES)
        offsets = [obs_ref[c : c + 1, lanes] - column_ref[rows, c : c + 1] for c in range(3)]
        square = offsets[0] * offsets[0] + offsets[1] * offsets[1] + offsets[2] * offsets[2]
        inverse = lax.rsqrt(square)
        cycles = square * inverse * (1.0 / (TIME * SPACING))

        sine, cosine = turn(cycles)
        sines, cosines = sine * cosine, 1.0 - sine * sine
        double = cosines + cosines
        fine = [(inverse, jnp.zeros_like(inverse)), (inverse * cosines, inverse * sines)]
        for n in range(2, 17):
            fine.append(tuple(double * fine[n - 1][i] - fine[n - 2][i] for i in range(2)))
        for n in range(17):
            fine_ref[16 + n, 0] = fine[n][0]
            fine_ref[16 + n, 1] = fine[n][1]
            if n:
                fine_ref[16 - n, 0] = fine[n][0]
                fine_ref[16 - n, 1] = -fine[n][1]

        sine, cosine = turn(cycles * 32.0)
        coarse = [(jnp.ones_like(inverse), jnp.zeros_like(inverse)), (1.0 - sine * sine, sine * cosine)]
        for n in range(1, 9):
            twice = coarse[n][0] + coarse[n][0]
            coarse.append((twice * coarse[n][0] - 1.0, twice * coarse[n][1]))
            if n < 8:
                coarse.append(
                    (twice * coarse[n + 1][0] - coarse[1][0], twice * coarse[n + 1][1] - coarse[1][1])
                )
        for n in range(17):
            coarse_ref[n, 0] = coarse[n][0]
            coarse_ref[n, 1] = coarse[n][1]

        @pl.when(step >= SLOTS)
        def _():
            wave_copy(held_ref, waves_ref, sem, slot, 0, 0).wait()

        for j in range(NF):
            bin_number = bins_smem[j]
            whole = (bin_number + 16) >> 5
            rest = bin_number - (whole << 5) + 16
            c0, s0 = coarse_ref[whole, 0], coarse_ref[whole, 1]
            c1, s1 = fine_ref[rest, 0], fine_ref[rest, 1]
            held_ref[slot, j, 0] = (c0 * c1 - s0 * s1).astype(jnp.bfloat16)
            held_ref[slot, j, 1] = (s0 * c1 + c0 * s1).astype(jnp.bfloat16)
        wave_copy(held_ref, waves_ref, sem, slot, row_tile, lane_tile).start()
        return carry

    steps = (LANES // TILE) * groups
    lax.fori_loop(0, steps, one_tile, 0)

    for slot in range(SLOTS):
        wave_copy(held_ref, waves_ref, sem, slot, 0, 0).wait()
    table_copy.wait()


def prepare(bins, place, counts, areas, obs, panel_position):
    observers = obs.shape[1]
    f32 = jnp.float32
    return pl.pallas_call(
        prepare_kernel,
        in_specs=[SMEM, SMEM, SMEM, HBM, VMEM, HBM],
        out_specs=[HBM] * 2 + [VMEM] * 3,
        out_shape=[
            pltpu.HBM((LANES // TILE, observers // LANES, NF, 2, TILE, LANES), jnp.bfloat16),
            pltpu.HBM((2 * NF, CHANNELS * TIME), jnp.bfloat16),
            jax.ShapeDtypeStruct((LANES, 8), f32),
            jax.ShapeDtypeStruct((8, LANES), f32),
            jax.ShapeDtypeStruct((1, LANES), f32),
        ],
        scratch_shapes=[
            pltpu.VMEM((33, 2, TILE, LANES), f32),
            pltpu.VMEM((17, 2, TILE, LANES), f32),
            pltpu.VMEM((SLOTS, NF, 2, TILE, LANES), jnp.bfloat16),
            pltpu.VMEM((2 * NF, CHANNELS * TIME), jnp.bfloat16),
            pltpu.SemaphoreType.DMA((SLOTS,)),
            pltpu.SemaphoreType.DMA,
            pltpu.VMEM(areas.shape, f32),
            pltpu.VMEM(panel_position.shape, f32),
            pltpu.SemaphoreType.DMA((2,)),
        ],
        cost_estimate=pl.CostEstimate(flops=20_000_000_000, bytes_accessed=40_000_000, transcendentals=0),
        compiler_params=pltpu.CompilerParams(vmem_limit_bytes=16 << 20),
        name="prepare",
    )(
        bins,
        place,
        counts,
        pltpu.with_memory_space_constraint(areas, pltpu.HBM),
        obs,
        pltpu.with_memory_space_constraint(panel_position, pltpu.HBM),
    )


def wave_fetch(waves_ref, held_ref, sem, b):
    return pltpu.make_async_copy(waves_ref.at[:, :, pl.ds(b * 4, 4)], held_ref.at[b], sem.at[b])


def radiate_kernel(
    bins_smem,
    data_in_ref,
    obs_ref,
    waves_ref,
    table_in_ref,
    column_ref,
    position_ref,
    scale_ref,
    o_ref,
    left_ref,
    product_ref,
    field_ref,
    inverse_ref,
    spread_ref,
    narrow_ref,
    table_ref,
    data_ref,
    source_ref,
    held_ref,
    sem,
    in_sem,
):
    table_copy = pltpu.make_async_copy(table_in_ref, narrow_ref, in_sem.at[0])
    table_copy.start()
    data_copy = pltpu.make_async_copy(data_in_ref, data_ref, in_sem.at[1])
    data_copy.start()
    for b in range(AHEAD):
        wave_fetch(waves_ref, held_ref, sem, b).start()
    rows = 2 * NF

    obs = obs_ref[...]
    high = obs.astype(jnp.bfloat16).astype(jnp.float32)
    low = obs - high
    minus = jnp.full((1, obs.shape[1]), -1.0, jnp.float32)
    factors = [v[c : c + 1] for v in (high, high, low) for c in range(3)] + [minus] * 6 + [minus * 0.0]
    spread_ref[...] = jnp.concatenate(
        [jnp.broadcast_to(v, (8, obs.shape[1])) for v in factors], axis=0
    ).astype(jnp.bfloat16)
    for group in range(obs_ref.shape[1] // LANES):
        lanes = slice(group * LANES, (group + 1) * LANES)
        offsets = [obs_ref[c : c + 1, lanes] - column_ref[:, c : c + 1] for c in range(3)]
        square = offsets[0] * offsets[0] + offsets[1] * offsets[1] + offsets[2] * offsets[2]
        inverse_ref[:, lanes] = lax.rsqrt(square)

    channel = lax.broadcasted_iota(jnp.int32, (16, LANES), 1) & 3
    table_copy.wait()
    for c in range(CHANNELS):
        mask = jnp.where(channel == (c + 1) % CHANNELS, 1.0, 0.0).astype(jnp.bfloat16)[0:1]
        for chunk in range(CHANNELS * TIME // LANES):
            lanes = slice(chunk * LANES, (chunk + 1) * LANES)
            table_ref[c * rows : (c + 1) * rows, lanes] = narrow_ref[:, lanes] * mask
    data_copy.wait()
    spectra = jnp.dot(table_ref[...], data_ref[...], preferred_element_type=jnp.float32)
    scales = [
        bins_of_block(bins_smem, b) * (2.0 * math.pi / (TIME * SPACING)) * scale_ref[...] for b in range(BLOCKS)
    ]
    spectra = spectra * jnp.concatenate(scales * CHANNELS, axis=0)
    row = lax.broadcasted_iota(jnp.int32, (8, LANES), 0)
    blank = jnp.zeros((8, 2 * LANES), jnp.float32)
    for b in range(BLOCKS):
        whole = spectra[192 + 8 * b : 200 + 8 * b]
        lead = whole.astype(jnp.bfloat16).astype(jnp.float32)
        rest = whole - lead
        for jj in range(4):
            real = jnp.where(row < 2, lead[jj : jj + 1], rest[jj : jj + 1])
            imag = jnp.where(row < 2, lead[4 + jj : 5 + jj], rest[4 + jj : 5 + jj])
            by_cosine = jnp.where(row % 2 == 0, -imag, real)
            by_sine = jnp.where(row % 2 == 0, real, imag)
            both = jnp.where(lax.broadcasted_iota(jnp.int32, (8, 2 * LANES), 0) < 4, jnp.concatenate([by_cosine, by_sine], axis=1), 0.0)
            source_ref[4 * b + jj] = jnp.concatenate([both, blank], axis=0).astype(jnp.bfloat16)
    for b in range(BLOCKS):
        direct = [spectra[c * rows + 8 * b : c * rows + 8 * b + 8] for c in range(3)]
        moment = [direct[c] * position_ref[c : c + 1, :] for c in range(3)]
        lead = [v.astype(jnp.bfloat16).astype(jnp.float32) for v in direct + moment]
        rest = [v - w for v, w in zip(direct + moment, lead)]
        slots = lead[:3] + rest[:3] + lead[:3] + lead[3:] + rest[3:] + [jnp.zeros((8, LANES), jnp.float32)]
        left_ref[b] = jnp.concatenate(slots, axis=0).T.astype(jnp.bfloat16)

    panels = inverse_ref.shape[0]
    width = 256

    def one_block(b, carry):
        @pl.when(b + AHEAD < BLOCKS)
        def _():
            wave_fetch(waves_ref, held_ref, sem, b + AHEAD).start()

        left = left_ref[b]
        lane = lax.broadcasted_iota(jnp.int32, (16, LANES), 1) & 7
        wave_fetch(waves_ref, held_ref, sem, b).wait()
        for jj in range(4):
            j = b * 4 + jj
            wave = jnp.full((8, LANES), bins_smem[j], jnp.int32).astype(jnp.float32)
            inverse_wave = 1.0 / (wave * (2.0 * math.pi / (TIME * SPACING)))
            source = source_ref[j]
            parts = [
                left * jnp.where(lane == s, 1.0, 0.0).astype(jnp.bfloat16)[0:1] for s in (jj, 4 + jj)
            ]
            for t in range(inverse_ref.shape[1] // width):
                parity = t % 2
                columns = slice(t * width, (t + 1) * width)
                for part in range(2):
                    product_ref[parity, part] = jnp.dot(
                        parts[part], spread_ref[:, columns], preferred_element_type=jnp.float32
                    )
                weights = jnp.concatenate(
                    [
                        jnp.concatenate([held_ref[b, i, 2 * t + half, jj, part] for half in range(2)], axis=1)
                        for part in range(2)
                        for i in range(panels // TILE)
                    ],
                    axis=0,
                )
                mono = jnp.dot(source, weights, preferred_element_type=jnp.float32)
                for half in range(2):
                    inner = slice(half * LANES, (half + 1) * LANES)
                    lane_tile = t * 2 + half
                    lanes = slice(lane_tile * LANES, (lane_tile + 1) * LANES)
                    far_real = far_imag = near_real = near_imag = jnp.zeros((8, LANES), jnp.float32)
                    for p in range(panels // 8):
                        rows = slice(p * 8, p * 8 + 8)
                        inverse = inverse_ref[rows, lanes]
                        if p % 2 == 0:
                            row_tile, inside = p * 8 // TILE, slice(p * 8 % TILE, p * 8 % TILE + 16)
                            cosines = held_ref[b, row_tile, lane_tile, jj, 0, inside].astype(jnp.float32)
                            sines = held_ref[b, row_tile, lane_tile, jj, 1, inside].astype(jnp.float32)
                        cosine = cosines[p % 2 * 8 : p % 2 * 8 + 8]
                        sine = sines[p % 2 * 8 : p % 2 * 8 + 8]
                        radial_real = product_ref[parity, 0, rows, inner] * inverse
                        radial_imag = product_ref[parity, 1, rows, inner] * inverse
                        term_real = cosine * radial_real + sine * radial_imag
                        term_imag = cosine * radial_imag - sine * radial_real
                        far_real = far_real + term_real
                        far_imag = far_imag + term_imag
                        near_real = near_real + inverse * term_real
                        near_imag = near_imag + inverse * term_imag
                    row = t * 4 + jj
                    sum_real = jnp.sum(near_real * inverse_wave - far_imag, axis=0, keepdims=True)
                    sum_imag = jnp.sum(near_imag * inverse_wave + far_real, axis=0, keepdims=True)
                    field_ref[b, 0, row : row + 1, inner] = sum_real + (mono[0:1, inner] + mono[2:3, inner])
                    field_ref[b, 1, row : row + 1, inner] = sum_imag + (mono[1:2, inner] + mono[3:4, inner])
        return carry

    lax.fori_loop(0, BLOCKS, one_block, 0)
    for part in range(2):
        flat = jnp.concatenate(
            [field_ref[b, part, 4 * t : 4 * t + 4] for t in range(4) for b in range(BLOCKS)], axis=0
        )
        o_ref[pl.ds(part, 2 * LANES, 2), :] = flat.T


def radiate(bins, data, observers, prepared, scale):
    panels, count = LANES, observers.shape[1]
    return pl.pallas_call(
        radiate_kernel,
        in_specs=[SMEM, pl.BlockSpec(memory_space=pl.ANY), VMEM, HBM, HBM, VMEM, VMEM, VMEM],
        out_specs=VMEM,
        out_shape=jax.ShapeDtypeStruct((count // 2, LANES), jnp.float32),
        scratch_shapes=[
            pltpu.VMEM((BLOCKS, panels, LANES), jnp.bfloat16),
            pltpu.VMEM((2, 2, panels, 256), jnp.float32),
            pltpu.VMEM((BLOCKS, 2, 16, 256), jnp.float32),
            pltpu.VMEM((panels, count), jnp.float32),
            pltpu.VMEM((LANES, count), jnp.bfloat16),
            pltpu.VMEM((2 * NF, CHANNELS * TIME), jnp.bfloat16),
            pltpu.VMEM((CHANNELS * 2 * NF, CHANNELS * TIME), jnp.bfloat16),
            pltpu.VMEM((CHANNELS * TIME, LANES), jnp.bfloat16),
            pltpu.VMEM((NF, 16, 2 * LANES), jnp.bfloat16),
            pltpu.VMEM((BLOCKS, panels // TILE, count // LANES, 4, 2, TILE, LANES), jnp.bfloat16),
            pltpu.SemaphoreType.DMA((BLOCKS,)),
            pltpu.SemaphoreType.DMA((2,)),
        ],
        cost_estimate=pl.CostEstimate(flops=20_000_000_000, bytes_accessed=40_000_000, transcendentals=0),
        compiler_params=pltpu.CompilerParams(vmem_limit_bytes=40 << 20),
        name="radiate",
    )(bins, data, observers, *prepared, scale)


def gather_kernel(x_ref, o_ref):
    total = jnp.zeros((8, LANES), jnp.float32)
    sums = [total, total, total, total]
    for i in range(x_ref.shape[0] // 8):
        sums[i % 4] = sums[i % 4] + x_ref[8 * i : 8 * i + 8, :]
    total = (sums[0] + sums[1]) + (sums[2] + sums[3])
    for part in range(2):
        whole = (total[part : part + 1] + total[part + 2 : part + 3]) + (
            total[part + 4 : part + 5] + total[part + 6 : part + 7]
        )
        for i in range(4):
            o_ref[part, i : i + 1, :] = whole[:, i * NF : (i + 1) * NF]


def gather(arrived):
    return pl.pallas_call(
        gather_kernel,
        in_specs=[VMEM],
        out_specs=VMEM,
        out_shape=jax.ShapeDtypeStruct((2, 4, NF), jnp.float32),
        name="gather",
    )(arrived)


def all_observers(obs_position):
    size = lax.axis_size("obs")
    local = jnp.transpose(obs_position.reshape(3, -1, 4), (0, 2, 1)).reshape(12, -1)
    held = [local]
    for shift in range(1, size):
        held.append(lax.ppermute(local, "obs", [((i + shift) % size, i) for i in range(size)]))
    own = lax.axis_index("obs")
    ring = jnp.stack(held + held)
    whole = lax.dynamic_slice_in_dim(ring, (size - own) % size, size, 0)
    return jnp.transpose(whole, (1, 2, 0)).reshape(3, -1)


def local_field(data, place, panel_position, panel_area, panel_counts, observers, bins):
    areas = panel_area.reshape(-1, LANES)
    prepared = prepare(bins, place, panel_counts, areas, observers, panel_position)
    waves, table, columns, position, scale = prepared
    held = [pltpu.with_memory_space_constraint(v, pltpu.HBM) for v in (waves, table)]
    return radiate(bins, data, observers, (*held, columns, position), scale)


def shards(samples, panel_position, panel_area, panel_counts, obs_position, freq_bins):
    arrived = lax.all_to_all(arrange(samples), ("panel", "obs"), 0, 0, tiled=True)
    data = arrived.reshape(-1, LANES)
    observers = all_observers(obs_position)

    place = lax.axis_index("obs")
    partial = local_field(
        data, place.reshape(1), panel_position, panel_area, panel_counts, observers, freq_bins
    )
    partial = partial.reshape(-1, 2, LANES)
    arrived = lax.all_to_all(partial, ("panel", "obs"), 0, 0, tiled=True)
    arrived = arrived.reshape(-1, LANES)
    return jnp.transpose(gather(arrived), (0, 2, 1))


def solution(mesh):
    in_specs = (
        P(("panel", "obs"), None, None),
        P(None, "panel"),
        P("panel"),
        P("panel"),
        P(None, "obs"),
        P(),
    )
    out_specs = P(None, None, ("obs", "panel"))
    return jax.shard_map(shards, mesh=mesh, in_specs=in_specs, out_specs=out_specs, check_vma=False)
```

```python
import math

import jax
import jax.numpy as jnp
from jax import lax
from jax.experimental import pallas as pl
from jax.experimental.pallas import tpu as pltpu
from jax.sharding import PartitionSpec as P


TIME = 1024
NF = 32
SPACING = 0.1
LANES = 128
CHANNELS = 4
AHEAD = 3
BLOCKS = 8
SLOTS = 4
TILE = 32

SIN_COEFFS = (
    4.442882919199695,
    -7.308245696158815,
    3.60635441147954,
    -0.8461128860931261,
    0.10982698817978952,
)
COS_COEFFS = (
    1.4142134965649862,
    -6.978850988235484,
    5.7394611706121585,
    -1.8835629868567052,
    0.31069819092073886,
)

VMEM = pl.BlockSpec(memory_space=pltpu.VMEM)
SMEM = pl.BlockSpec(memory_space=pltpu.SMEM)
HBM = pl.BlockSpec(memory_space=pltpu.HBM)


def horner(square, coeffs):
    total = square * coeffs[-1] + coeffs[-2]
    for coeff in coeffs[-3::-1]:
        total = total * square + coeff
    return total


def turn(cycles):
    part = cycles - jnp.round(cycles)
    square = part * part
    return part * horner(square, SIN_COEFFS), horner(square, COS_COEFFS)


def arrange_kernel(x_ref, o_ref, held_ref, made_ref, sem, out_sem):
    pieces, steps, _, piece = held_ref.shape
    copies = [
        pltpu.make_async_copy(x_ref.at[:, :, i * piece : (i + 1) * piece], held_ref.at[i], sem.at[i])
        for i in range(pieces)
    ]
    for copy in copies:
        copy.start()
    blocks = piece // LANES

    def outward(i):
        done = pl.ds(i * blocks, blocks)
        return pltpu.make_async_copy(made_ref.at[done], o_ref.at[done], out_sem.at[i])

    for i, copy in enumerate(copies):
        copy.wait()
        for block in range(blocks):
            for step in range(steps):
                made_ref[i * blocks + block, step] = held_ref[i, step, :, block * LANES : (block + 1) * LANES]
        outward(i).start()
    for i in range(pieces):
        outward(i).wait()


def arrange(samples):
    steps, channels, panels = samples.shape
    pieces = 4
    return pl.pallas_call(
        arrange_kernel,
        in_specs=[HBM],
        out_specs=HBM,
        out_shape=pltpu.HBM((panels // LANES, steps, channels, LANES), samples.dtype),
        scratch_shapes=[
            pltpu.VMEM((pieces, steps, channels, panels // pieces), samples.dtype),
            pltpu.VMEM((panels // LANES, steps, channels, LANES), samples.dtype),
            pltpu.SemaphoreType.DMA((pieces,)),
            pltpu.SemaphoreType.DMA((pieces,)),
        ],
        compiler_params=pltpu.CompilerParams(vmem_limit_bytes=8 << 20),
        name="arrange",
    )(pltpu.with_memory_space_constraint(samples, pltpu.HBM))


def bins_of_block(bins_smem, b):
    row = lax.broadcasted_iota(jnp.int32, (8, LANES), 0) % 4
    bins = [jnp.full((8, LANES), bins_smem[4 * b + i], jnp.int32) for i in range(4)]
    chosen = jnp.where(row == 0, bins[0], jnp.where(row == 1, bins[1], jnp.where(row == 2, bins[2], bins[3])))
    return chosen.astype(jnp.float32)


def wave_copy(held_ref, waves_ref, sem, slot, rows, lanes):
    return pltpu.make_async_copy(held_ref.at[slot], waves_ref.at[rows, lanes], sem.at[slot])


def prepare_kernel(
    bins_smem,
    place_smem,
    obs_ref,
    panel_ref,
    waves_ref,
    table_out_ref,
    column_ref,
    position_ref,
    fine_ref,
    coarse_ref,
    held_ref,
    table_ref,
    sem,
    table_sem,
):
    start = pl.multiple_of(place_smem[0] * LANES, LANES)
    mine = panel_ref[:, pl.ds(start, LANES)]
    position_ref[...] = jnp.concatenate([mine, jnp.zeros((5, LANES), jnp.float32)], axis=0)
    column_ref[...] = position_ref[...].T

    def one_chunk(chunk, carry):
        start = pl.multiple_of(chunk * LANES, LANES)
        time = ((lax.broadcasted_iota(jnp.int32, (8, LANES), 1) + start) >> 2).astype(jnp.float32)
        sine, cosine = turn(time * (1.0 / TIME))
        weight = (2.0 / TIME) * (0.5 * (sine * sine))
        is_real = lax.broadcasted_iota(jnp.int32, (8, LANES), 0) < 4
        values = []
        for b in range(BLOCKS):
            sine, cosine = turn(bins_of_block(bins_smem, b) * time * (1.0 / TIME))
            values.append(weight * jnp.where(is_real, 1.0 - sine * sine, -(sine * cosine)))
        table_ref[:, pl.ds(start, LANES)] = jnp.concatenate(values, axis=0).astype(jnp.bfloat16)
        return carry

    lax.fori_loop(0, TIME * CHANNELS // LANES, one_chunk, 0)
    table_copy = pltpu.make_async_copy(table_ref, table_out_ref, table_sem)
    table_copy.start()

    groups = obs_ref.shape[1] // LANES

    def one_tile(step, carry):
        row_tile, lane_tile, slot = step // groups, step % groups, step % SLOTS
        rows = pl.ds(pl.multiple_of(row_tile * TILE, TILE), TILE)
        lanes = pl.ds(pl.multiple_of(lane_tile * LANES, LANES), LANES)
        offsets = [obs_ref[c : c + 1, lanes] - column_ref[rows, c : c + 1] for c in range(3)]
        square = offsets[0] * offsets[0] + offsets[1] * offsets[1] + offsets[2] * offsets[2]
        inverse = lax.rsqrt(square)
        cycles = square * inverse * (1.0 / (TIME * SPACING))

        sine, cosine = turn(cycles)
        sines, cosines = sine * cosine, 1.0 - sine * sine
        double = cosines + cosines
        fine = [(inverse, jnp.zeros_like(inverse)), (inverse * cosines, inverse * sines)]
        for n in range(2, 17):
            fine.append(tuple(double * fine[n - 1][i] - fine[n - 2][i] for i in range(2)))
        for n in range(17):
            fine_ref[16 + n, 0] = fine[n][0]
            fine_ref[16 + n, 1] = fine[n][1]
            if n:
                fine_ref[16 - n, 0] = fine[n][0]
                fine_ref[16 - n, 1] = -fine[n][1]

        sine, cosine = turn(cycles * 32.0)
        coarse = [(jnp.ones_like(inverse), jnp.zeros_like(inverse)), (1.0 - sine * sine, sine * cosine)]
        for n in range(1, 9):
            twice = coarse[n][0] + coarse[n][0]
            coarse.append((twice * coarse[n][0] - 1.0, twice * coarse[n][1]))
            if n < 8:
                coarse.append(
                    (twice * coarse[n + 1][0] - coarse[1][0], twice * coarse[n + 1][1] - coarse[1][1])
                )
        for n in range(17):
            coarse_ref[n, 0] = coarse[n][0]
            coarse_ref[n, 1] = coarse[n][1]

        @pl.when(step >= SLOTS)
        def _():
            wave_copy(held_ref, waves_ref, sem, slot, 0, 0).wait()

        for j in range(NF):
            bin_number = bins_smem[j]
            whole = (bin_number + 16) >> 5
            rest = bin_number - (whole << 5) + 16
            c0, s0 = coarse_ref[whole, 0], coarse_ref[whole, 1]
            c1, s1 = fine_ref[rest, 0], fine_ref[rest, 1]
            held_ref[slot, j, 0] = (c0 * c1 - s0 * s1).astype(jnp.bfloat16)
            held_ref[slot, j, 1] = (s0 * c1 + c0 * s1).astype(jnp.bfloat16)
        wave_copy(held_ref, waves_ref, sem, slot, row_tile, lane_tile).start()
        return carry

    steps = (LANES // TILE) * groups
    lax.fori_loop(0, steps, one_tile, 0)

    for slot in range(SLOTS):
        wave_copy(held_ref, waves_ref, sem, slot, 0, 0).wait()
    table_copy.wait()


def prepare(bins, place, obs, panel_position):
    observers = obs.shape[1]
    f32 = jnp.float32
    return pl.pallas_call(
        prepare_kernel,
        in_specs=[SMEM, SMEM, VMEM, VMEM],
        out_specs=[HBM] * 2 + [VMEM] * 2,
        out_shape=[
            pltpu.HBM((LANES // TILE, observers // LANES, NF, 2, TILE, LANES), jnp.bfloat16),
            pltpu.HBM((2 * NF, CHANNELS * TIME), jnp.bfloat16),
            jax.ShapeDtypeStruct((LANES, 8), f32),
            jax.ShapeDtypeStruct((8, LANES), f32),
        ],
        scratch_shapes=[
            pltpu.VMEM((33, 2, TILE, LANES), f32),
            pltpu.VMEM((17, 2, TILE, LANES), f32),
            pltpu.VMEM((SLOTS, NF, 2, TILE, LANES), jnp.bfloat16),
            pltpu.VMEM((2 * NF, CHANNELS * TIME), jnp.bfloat16),
            pltpu.SemaphoreType.DMA((SLOTS,)),
            pltpu.SemaphoreType.DMA,
        ],
        cost_estimate=pl.CostEstimate(flops=20_000_000_000, bytes_accessed=40_000_000, transcendentals=0),
        compiler_params=pltpu.CompilerParams(vmem_limit_bytes=16 << 20),
        name="prepare",
    )(bins, place, obs, panel_position)


def wave_fetch(waves_ref, held_ref, sem, b):
    return pltpu.make_async_copy(waves_ref.at[:, :, pl.ds(b * 4, 4)], held_ref.at[b], sem.at[b])


def radiate_kernel(
    bins_smem,
    data_in_ref,
    obs_ref,
    waves_ref,
    table_in_ref,
    column_ref,
    position_ref,
    scale_ref,
    o_ref,
    left_ref,
    product_ref,
    field_ref,
    inverse_ref,
    spread_ref,
    narrow_ref,
    table_ref,
    data_ref,
    source_ref,
    held_ref,
    sem,
    in_sem,
):
    table_copy = pltpu.make_async_copy(table_in_ref, narrow_ref, in_sem.at[0])
    table_copy.start()
    data_copy = pltpu.make_async_copy(data_in_ref, data_ref, in_sem.at[1])
    data_copy.start()
    for b in range(AHEAD):
        wave_fetch(waves_ref, held_ref, sem, b).start()
    rows = 2 * NF

    obs = obs_ref[...]
    high = obs.astype(jnp.bfloat16).astype(jnp.float32)
    low = obs - high
    minus = jnp.full((1, obs.shape[1]), -1.0, jnp.float32)
    factors = [v[c : c + 1] for v in (high, high, low) for c in range(3)] + [minus] * 6 + [minus * 0.0]
    spread_ref[...] = jnp.concatenate(
        [jnp.broadcast_to(v, (8, obs.shape[1])) for v in factors], axis=0
    ).astype(jnp.bfloat16)
    for group in range(obs_ref.shape[1] // LANES):
        lanes = slice(group * LANES, (group + 1) * LANES)
        offsets = [obs_ref[c : c + 1, lanes] - column_ref[:, c : c + 1] for c in range(3)]
        square = offsets[0] * offsets[0] + offsets[1] * offsets[1] + offsets[2] * offsets[2]
        inverse_ref[:, lanes] = lax.rsqrt(square)

    channel = lax.broadcasted_iota(jnp.int32, (16, LANES), 1) & 3
    table_copy.wait()
    for c in range(CHANNELS):
        mask = jnp.where(channel == (c + 1) % CHANNELS, 1.0, 0.0).astype(jnp.bfloat16)[0:1]
        for chunk in range(CHANNELS * TIME // LANES):
            lanes = slice(chunk * LANES, (chunk + 1) * LANES)
            table_ref[c * rows : (c + 1) * rows, lanes] = narrow_ref[:, lanes] * mask
    data_copy.wait()
    spectra = jnp.dot(table_ref[...], data_ref[...], preferred_element_type=jnp.float32)
    scales = [
        bins_of_block(bins_smem, b) * (2.0 * math.pi / (TIME * SPACING)) * scale_ref[...] for b in range(BLOCKS)
    ]
    spectra = spectra * jnp.concatenate(scales * CHANNELS, axis=0)
    row = lax.broadcasted_iota(jnp.int32, (8, LANES), 0)
    blank = jnp.zeros((8, 2 * LANES), jnp.float32)
    for b in range(BLOCKS):
        whole = spectra[192 + 8 * b : 200 + 8 * b]
        lead = whole.astype(jnp.bfloat16).astype(jnp.float32)
        rest = whole - lead
        for jj in range(4):
            real = jnp.where(row < 2, lead[jj : jj + 1], rest[jj : jj + 1])
            imag = jnp.where(row < 2, lead[4 + jj : 5 + jj], rest[4 + jj : 5 + jj])
            by_cosine = jnp.where(row % 2 == 0, -imag, real)
            by_sine = jnp.where(row % 2 == 0, real, imag)
            both = jnp.where(lax.broadcasted_iota(jnp.int32, (8, 2 * LANES), 0) < 4, jnp.concatenate([by_cosine, by_sine], axis=1), 0.0)
            source_ref[4 * b + jj] = jnp.concatenate([both, blank], axis=0).astype(jnp.bfloat16)
    for b in range(BLOCKS):
        direct = [spectra[c * rows + 8 * b : c * rows + 8 * b + 8] for c in range(3)]
        moment = [direct[c] * position_ref[c : c + 1, :] for c in range(3)]
        lead = [v.astype(jnp.bfloat16).astype(jnp.float32) for v in direct + moment]
        rest = [v - w for v, w in zip(direct + moment, lead)]
        slots = lead[:3] + rest[:3] + lead[:3] + lead[3:] + rest[3:] + [jnp.zeros((8, LANES), jnp.float32)]
        left_ref[b] = jnp.concatenate(slots, axis=0).T.astype(jnp.bfloat16)

    panels = inverse_ref.shape[0]
    width = 256

    def one_block(b, carry):
        @pl.when(b + AHEAD < BLOCKS)
        def _():
            wave_fetch(waves_ref, held_ref, sem, b + AHEAD).start()

        left = left_ref[b]
        lane = lax.broadcasted_iota(jnp.int32, (16, LANES), 1) & 7
        wave_fetch(waves_ref, held_ref, sem, b).wait()
        for jj in range(4):
            j = b * 4 + jj
            wave = jnp.full((8, LANES), bins_smem[j], jnp.int32).astype(jnp.float32)
            inverse_wave = 1.0 / (wave * (2.0 * math.pi / (TIME * SPACING)))
            source = source_ref[j]
            parts = [
                left * jnp.where(lane == s, 1.0, 0.0).astype(jnp.bfloat16)[0:1] for s in (jj, 4 + jj)
            ]
            for t in range(inverse_ref.shape[1] // width):
                parity = t % 2
                columns = slice(t * width, (t + 1) * width)
                for part in range(2):
                    product_ref[parity, part] = jnp.dot(
                        parts[part], spread_ref[:, columns], preferred_element_type=jnp.float32
                    )
                weights = jnp.concatenate(
                    [
                        jnp.concatenate([held_ref[b, i, 2 * t + half, jj, part] for half in range(2)], axis=1)
                        for part in range(2)
                        for i in range(panels // TILE)
                    ],
                    axis=0,
                )
                mono = jnp.dot(source, weights, preferred_element_type=jnp.float32)
                for half in range(2):
                    inner = slice(half * LANES, (half + 1) * LANES)
                    lane_tile = t * 2 + half
                    lanes = slice(lane_tile * LANES, (lane_tile + 1) * LANES)
                    far_real = far_imag = near_real = near_imag = jnp.zeros((8, LANES), jnp.float32)
                    for p in range(panels // 8):
                        rows = slice(p * 8, p * 8 + 8)
                        inverse = inverse_ref[rows, lanes]
                        if p % 2 == 0:
                            row_tile, inside = p * 8 // TILE, slice(p * 8 % TILE, p * 8 % TILE + 16)
                            cosines = held_ref[b, row_tile, lane_tile, jj, 0, inside].astype(jnp.float32)
                            sines = held_ref[b, row_tile, lane_tile, jj, 1, inside].astype(jnp.float32)
                        cosine = cosines[p % 2 * 8 : p % 2 * 8 + 8]
                        sine = sines[p % 2 * 8 : p % 2 * 8 + 8]
                        radial_real = product_ref[parity, 0, rows, inner] * inverse
                        radial_imag = product_ref[parity, 1, rows, inner] * inverse
                        term_real = cosine * radial_real + sine * radial_imag
                        term_imag = cosine * radial_imag - sine * radial_real
                        far_real = far_real + term_real
                        far_imag = far_imag + term_imag
                        near_real = near_real + inverse * term_real
                        near_imag = near_imag + inverse * term_imag
                    row = t * 4 + jj
                    sum_real = jnp.sum(near_real * inverse_wave - far_imag, axis=0, keepdims=True)
                    sum_imag = jnp.sum(near_imag * inverse_wave + far_real, axis=0, keepdims=True)
                    field_ref[b, 0, row : row + 1, inner] = sum_real + (mono[0:1, inner] + mono[2:3, inner])
                    field_ref[b, 1, row : row + 1, inner] = sum_imag + (mono[1:2, inner] + mono[3:4, inner])
        return carry

    lax.fori_loop(0, BLOCKS, one_block, 0)
    for part in range(2):
        flat = jnp.concatenate(
            [field_ref[b, part, 4 * t : 4 * t + 4] for t in range(4) for b in range(BLOCKS)], axis=0
        )
        o_ref[pl.ds(part, 2 * LANES, 2), :] = flat.T


def radiate(bins, data, observers, prepared, scale):
    panels, count = LANES, observers.shape[1]
    return pl.pallas_call(
        radiate_kernel,
        in_specs=[SMEM, pl.BlockSpec(memory_space=pl.ANY), VMEM, HBM, HBM, VMEM, VMEM, VMEM],
        out_specs=VMEM,
        out_shape=jax.ShapeDtypeStruct((count // 2, LANES), jnp.float32),
        scratch_shapes=[
            pltpu.VMEM((BLOCKS, panels, LANES), jnp.bfloat16),
            pltpu.VMEM((2, 2, panels, 256), jnp.float32),
            pltpu.VMEM((BLOCKS, 2, 16, 256), jnp.float32),
            pltpu.VMEM((panels, count), jnp.float32),
            pltpu.VMEM((LANES, count), jnp.bfloat16),
            pltpu.VMEM((2 * NF, CHANNELS * TIME), jnp.bfloat16),
            pltpu.VMEM((CHANNELS * 2 * NF, CHANNELS * TIME), jnp.bfloat16),
            pltpu.VMEM((CHANNELS * TIME, LANES), jnp.bfloat16),
            pltpu.VMEM((NF, 16, 2 * LANES), jnp.bfloat16),
            pltpu.VMEM((BLOCKS, panels // TILE, count // LANES, 4, 2, TILE, LANES), jnp.bfloat16),
            pltpu.SemaphoreType.DMA((BLOCKS,)),
            pltpu.SemaphoreType.DMA((2,)),
        ],
        cost_estimate=pl.CostEstimate(flops=20_000_000_000, bytes_accessed=40_000_000, transcendentals=0),
        compiler_params=pltpu.CompilerParams(vmem_limit_bytes=40 << 20),
        name="radiate",
    )(bins, data, observers, *prepared, scale)


def gather_kernel(x_ref, o_ref):
    total = jnp.zeros((8, LANES), jnp.float32)
    sums = [total, total, total, total]
    for i in range(x_ref.shape[0] // 8):
        sums[i % 4] = sums[i % 4] + x_ref[8 * i : 8 * i + 8, :]
    total = (sums[0] + sums[1]) + (sums[2] + sums[3])
    for part in range(2):
        whole = (total[part : part + 1] + total[part + 2 : part + 3]) + (
            total[part + 4 : part + 5] + total[part + 6 : part + 7]
        )
        for i in range(4):
            o_ref[part, i : i + 1, :] = whole[:, i * NF : (i + 1) * NF]


def gather(arrived):
    return pl.pallas_call(
        gather_kernel,
        in_specs=[VMEM],
        out_specs=VMEM,
        out_shape=jax.ShapeDtypeStruct((2, 4, NF), jnp.float32),
        name="gather",
    )(arrived)


def all_observers(obs_position):
    size = lax.axis_size("obs")
    local = jnp.transpose(obs_position.reshape(3, -1, 4), (0, 2, 1)).reshape(12, -1)
    held = [local]
    for shift in range(1, size):
        held.append(lax.ppermute(local, "obs", [((i + shift) % size, i) for i in range(size)]))
    own = lax.axis_index("obs")
    ring = jnp.stack(held + held)
    whole = lax.dynamic_slice_in_dim(ring, (size - own) % size, size, 0)
    return jnp.transpose(whole, (1, 2, 0)).reshape(3, -1)


def local_field(data, place, panel_position, scale, observers, bins):
    prepared = prepare(bins, place, observers, panel_position)
    waves, table, columns, position = prepared
    held = [pltpu.with_memory_space_constraint(v, pltpu.HBM) for v in (waves, table)]
    return radiate(bins, data, observers, (*held, columns, position), scale)


def shards(samples, panel_position, panel_area, panel_counts, obs_position, freq_bins):
    arrived = lax.all_to_all(arrange(samples), ("panel", "obs"), 0, 0, tiled=True)
    data = arrived.reshape(-1, LANES)
    observers = all_observers(obs_position)

    place = lax.axis_index("obs")
    area = lax.dynamic_slice_in_dim(panel_area, place * LANES, LANES, 0)
    count = lax.dynamic_slice_in_dim(panel_counts, place, 1, 0)
    lane_ids = jnp.arange(LANES, dtype=jnp.int32)
    scale = jnp.where(lane_ids < count, area * (1.0 / (4.0 * math.pi)), 0.0)[None, :]

    partial = local_field(data, place.reshape(1), panel_position, scale, observers, freq_bins)
    partial = partial.reshape(-1, 2, LANES)
    arrived = lax.all_to_all(partial, ("panel", "obs"), 0, 0, tiled=True)
    arrived = arrived.reshape(-1, LANES)
    return jnp.transpose(gather(arrived), (0, 2, 1))


def solution(mesh):
    in_specs = (
        P(("panel", "obs"), None, None),
        P(None, "panel"),
        P("panel"),
        P("panel"),
        P(None, "obs"),
        P(),
    )
    out_specs = P(None, None, ("obs", "panel"))
    return jax.shard_map(shards, mesh=mesh, in_specs=in_specs, out_specs=out_specs, check_vma=False)
```
